8 devices in a mesh: dp: 2 (over y, z), sp: 4 (over x, core).
Axes of the slice: x: 2, y: 2, z: 1, core: 2. Of those that a mesh axis runs over, the one named last changes fastest.
Arguments:
- x: bfloat16 [16384, 2048], P(('dp', 'sp')), parts along dimension 0
- gain: bfloat16 [2048], replicated
- wq: bfloat16 [2048, 2048], P('sp')
- wk: bfloat16 [2048, 2048], P('sp')
- wv: bfloat16 [2048, 2048], P('sp')
- wo: bfloat16 [2048, 2048], P('sp')
Outputs:
- output: bfloat16 [16384, 2048], P(('dp', 'sp')), parts along dimension 0
There are 2 independent parts. The reference program is written for one: setup_inputs(seed, part) draws one part's arguments, and reference() takes and returns one part's arrays. A program takes and returns all parts, laid end to end along the dimension named above; an argument that names none is the same for every part.
All inputs are finite; a program needn't handle non-finite values.
Results may differ from the reference program's by a relative error of at most 0.012.
Values are sent between devices in bfloat16 or wider.
A program may use at most 2 GiB of HBM per device.

```python
import jax
import jax.numpy as jnp
from jax import lax

ROWS = 8192
D = 2048
HEADS = 8
KV_HEADS = 8
HEAD = 256
THETA = 10000


def setup_inputs(seed: int = 0, part: int = 0) -> dict:
    kx, kn, kq, kk, kv, ko = jax.random.split(jax.random.key(seed), 6)

    def weights(key, rows, columns):
        return jax.random.normal(key, (rows, columns), jnp.float32) * rows**-0.5

    drawn = {
        "x": jax.random.normal(jax.random.fold_in(kx, part), (ROWS, D), jnp.float32),
        "gain": 1 + 0.1 * jax.random.normal(kn, (D,), jnp.float32),
        "wq": 2 * weights(kq, D, HEADS * HEAD),
        "wk": 2 * weights(kk, D, KV_HEADS * HEAD),
        "wv": 4 * weights(kv, D, KV_HEADS * HEAD),
        "wo": weights(ko, HEADS * HEAD, D),
    }
    return {k: v.astype(jnp.bfloat16) for k, v in drawn.items()}


def normed(x, gain):
    wide = x.astype(jnp.float32)
    scale = lax.rsqrt(jnp.mean(wide * wide, -1, keepdims=True) + 1e-6)
    return (wide * scale * gain.astype(jnp.float32)).astype(jnp.bfloat16)


def turned(t, place, theta):
    half = t.shape[-1] // 2
    angle = place.astype(jnp.float32)[:, None] * theta ** (-jnp.arange(half, dtype=jnp.float32) / half)
    cos, sin = jnp.cos(angle)[:, None], jnp.sin(angle)[:, None]
    a, b = t[..., :half].astype(jnp.float32), t[..., half:].astype(jnp.float32)
    return jnp.concatenate([a * cos - b * sin, b * cos + a * sin], -1).astype(jnp.bfloat16)


def matmul(a, w):
    return jnp.dot(a, w, preferred_element_type=jnp.float32).astype(jnp.bfloat16)


def einsum(form, a, b):
    return jnp.einsum(form, a.astype(jnp.float32), b.astype(jnp.float32))


def attention(q, k, v):
    scores = einsum("tgsd,ugd->gstu", q, k) * q.shape[-1] ** -0.5
    token = jnp.arange(q.shape[0])
    scores = jnp.where(token[:, None] >= token, scores, -jnp.inf)
    weights = jax.nn.softmax(scores, -1).astype(jnp.bfloat16)
    return einsum("gstu,ugd->tgsd", weights, v).astype(jnp.bfloat16)


def reference(x, gain, wq, wk, wv, wo):
    a, place = normed(x, gain), jnp.arange(ROWS)
    q = turned(matmul(a, wq).reshape(ROWS, HEADS, HEAD), place, THETA).reshape(ROWS, KV_HEADS, -1, HEAD)
    k = turned(matmul(a, wk).reshape(ROWS, KV_HEADS, HEAD), place, THETA)
    v = matmul(a, wv).reshape(ROWS, KV_HEADS, HEAD)
    seen = attention(q, k, v).reshape(ROWS, HEADS * HEAD)
    return (x.astype(jnp.float32) + jnp.dot(seen, wo, preferred_element_type=jnp.float32)).astype(jnp.bfloat16)
```

```python
import functools

import jax
import jax.numpy as jnp
from jax import lax
from jax.experimental import pallas as pl
from jax.experimental.pallas import tpu as pltpu
from jax.sharding import PartitionSpec as P

NEG = -1e30
HIDDEN = 2 * NEG
LOG2E = 1.4426950408889634
HEAD = 256
HEADS = 8
OWN = 4
D = 2048
TOK = 2048
CHIP = 2 * TOK
PIECE = D // 4
HALF = PIECE // 2
NCH = 4
CH = HALF // NCH
STRIP = 512
NS = CHIP // STRIP
THETA = 10000
SCALE = HEAD**-0.5
MESH = pl.DeviceIdType.MESH
VMEM = 63 * 2**20
F32, BF16 = jnp.float32, jnp.bfloat16


def _places():
    dp, s = lax.axis_index("dp"), lax.axis_index("sp")
    core = lax.rem(s, 2)
    s1 = s + 1 - 2 * core
    s2, s3 = lax.rem(s + 2, 4), lax.rem(s1 + 2, 4)
    return dp, s, core, s1, s2, s3


def _greet(devices):
    barrier = pltpu.get_barrier_semaphore()
    for d in devices:
        pl.semaphore_signal(barrier, inc=1, device_id=d, device_id_type=MESH)
    pl.semaphore_wait(barrier, len(devices))


def _dot(a, b):
    return jnp.dot(a, b, preferred_element_type=F32)


def _project(x_ref, gain_ref, cos_ref, sin_ref, wq_ref, wk_ref, wv_ref, wo_ref, qt_ref, k_ref, vt_ref, rest_ref,
             a_s, x_s, w_s, t_s, k_s, x_sem, l_sem, os_sem, or_sem, xs_sem, xr_sem, ys_sem, yr_sem, ds_sem, dr_sem, es_sem, er_sem,
             slot_sem, to_sem):
    dp, s, core, s1, s2, s3 = _places()
    w_refs = (wq_ref, wk_ref, wv_ref, wo_ref)
    beside, across, other = (dp, s1), (dp, s2), (1 - dp, s)
    _greet((beside, across, other))

    def held(m, row, n):
        return w_s.at[m, pl.ds(row, n)] if m < 3 else rest_ref.at[pl.ds(row - PIECE, n)]

    def remote(src, dst, send, recv, device):
        return pltpu.make_async_remote_copy(src_ref=src, dst_ref=dst, send_sem=send, recv_sem=recv, device_id=device, device_id_type=MESH)

    def own_copy(m):
        return remote(w_refs[m], held(m, PIECE, PIECE), os_sem.at[m], or_sem.at[m], beside)

    def x_copy(m, n):
        at = dp * HALF + n * CH
        return remote(w_refs[m].at[pl.ds(at, CH)], held(m, 2 * PIECE + at, CH), xs_sem.at[m, n], xr_sem.at[m, n], across)

    def y_copy(m, n):
        at = 2 * PIECE + dp * HALF + n * CH
        return remote(held(m, at, CH), held(m, at, CH), ys_sem.at[m, n], yr_sem.at[m, n], other)

    def d_copy(m, n):
        at = dp * HALF + n * CH
        return remote(held(m, 2 * PIECE + at, CH), held(m, 3 * PIECE + at, CH), ds_sem.at[m, n], dr_sem.at[m, n], beside)

    def e_copy(m, n):
        at = (1 - dp) * HALF + n * CH
        return remote(held(m, 2 * PIECE + at, CH), held(m, 3 * PIECE + at, CH), es_sem.at[m, n], er_sem.at[m, n], beside)

    def local_copy(m):
        return pltpu.make_async_copy(w_refs[m], w_s.at[m, pl.ds(0, PIECE)], l_sem.at[m])

    def pass_x(m, n):
        x_copy(m, n).wait_recv()
        y_copy(m, n).start()
        d_copy(m, n).start()

    def pass_y(m, n):
        y_copy(m, n).wait_recv()
        e_copy(m, n).start()

    def ready(m):
        own_copy(m).wait_recv()
        for n in range(NCH):
            d_copy(m, n).wait_recv()
            e_copy(m, n).wait_recv()
        if m < 3:
            local_copy(m).wait()

    XR = x_s.shape[1]
    steps = TOK // XR

    def x_in(n):
        return pltpu.make_async_copy(x_ref.at[pl.ds(n * XR, XR)], x_s.at[lax.rem(n, 2)], x_sem.at[lax.rem(n, 2)])

    x_in(0).start()
    for m in range(4):
        for n in range(NCH):
            x_copy(m, n).start()
        own_copy(m).start()
        if m < 3:
            local_copy(m).start()

    def norm(n, _):
        @pl.when(n + 1 < steps)
        def _():
            x_in(n + 1).start()

        x_in(n).wait()
        slot = lax.rem(n, 2)
        wide = x_s[slot].astype(F32)
        scale = lax.rsqrt(jnp.mean(wide * wide, -1, keepdims=True) + 1e-6)
        for j, p in enumerate((s, s1, s2, s3)):
            cols = pl.ds(pl.multiple_of(p * PIECE, PIECE), PIECE)
            a = x_s[slot, :, cols].astype(F32) * scale * gain_ref[:, cols].astype(F32)
            a_s[pl.ds(pl.multiple_of(n * XR, XR), XR), j * PIECE : (j + 1) * PIECE] = a.astype(BF16)

    lax.fori_loop(0, steps, norm, None)
    for n in range(NCH):
        pass_x(0, n)
    for n in range(NCH):
        pass_y(0, n)

    outs = (qt_ref, k_ref, vt_ref)
    here = pl.ds(pl.multiple_of(core * TOK, TOK), TOK)

    def stage(m):
        return k_s if m == 1 else t_s

    def out(m, n):
        return outs[m].at[n, here, :] if m == 1 else outs[m].at[n, :, here]

    def sent(m, n):
        return remote(stage(m).at[n], out(m, n), slot_sem.at[m, n], to_sem.at[m, n], beside)

    def kept(m, n):
        return pltpu.make_async_copy(stage(m).at[OWN + n], out(m, n), slot_sem.at[m, OWN + n])

    def make(m, h, slot):
        cols = pl.ds(pl.multiple_of(h * HEAD, HEAD), HEAD)

        def strip(r, _):
            rows = pl.ds(pl.multiple_of(r * STRIP, STRIP), STRIP)
            t = _dot(a_s[rows, :], w_s[m, :, cols]).astype(BF16)
            if m < 2:
                t = t.astype(F32)
                lo, hi = t[:, : HEAD // 2], t[:, HEAD // 2 :]
                cos, sin = cos_ref[rows, :], sin_ref[rows, :]
                t = jnp.concatenate([lo * cos - hi * sin, hi * cos + lo * sin], axis=1).astype(BF16)
            if m == 1:
                k_s[slot, rows, :] = t
            else:
                t_s[slot, :, rows] = t.T

        lax.fori_loop(0, TOK // STRIP, strip, None)

    for m in range(3):
        ready(m)

        def away(n, _):
            if m == 2:
                sent(0, n).wait_send()
            make(m, (1 - core) * OWN + n, n)
            sent(m, n).start()
            pass_x(m + 1, n)

        def home(n, _):
            if m == 2:
                kept(0, n).wait()
            pass_y(m + 1, n)
            make(m, core * OWN + n, OWN + n)
            kept(m, n).start()

        lax.fori_loop(0, OWN, away, None)
        lax.fori_loop(0, OWN, home, None)

    ready(3)
    for m in range(4):
        own_copy(m).wait_send()
        for n in range(NCH):
            x_copy(m, n).wait_send()
            y_copy(m, n).wait_send()
            d_copy(m, n).wait_send()
            e_copy(m, n).wait_send()
    for m in range(3):
        for n in range(OWN):
            if m > 0:
                sent(m, n).wait_send()
                kept(m, n).wait()
            sent(m, n).wait_recv()


def project(x, gain, cos, sin, wq, wk, wv, wo):
    hbm, vmem = pl.BlockSpec(memory_space=pltpu.HBM), pl.BlockSpec(memory_space=pltpu.VMEM)
    dma = pltpu.SemaphoreType.DMA
    return pl.pallas_call(
        _project,
        in_specs=[hbm, vmem, vmem, vmem, hbm, hbm, hbm, hbm],
        out_specs=[hbm] * 4,
        out_shape=[
            jax.ShapeDtypeStruct((OWN, HEAD, CHIP), BF16),
            jax.ShapeDtypeStruct((OWN, CHIP, HEAD), BF16),
            jax.ShapeDtypeStruct((OWN, HEAD, CHIP), BF16),
            jax.ShapeDtypeStruct((3 * PIECE, D), BF16),
        ],
        scratch_shapes=[
            pltpu.VMEM((TOK, D), BF16),
            pltpu.VMEM((2, 256, D), BF16),
            pltpu.VMEM((3, D, D), BF16),
            pltpu.VMEM((2 * OWN, HEAD, TOK), BF16),
            pltpu.VMEM((2 * OWN, TOK, HEAD), BF16),
            dma((2,)), dma((3,)), dma((4,)), dma((4,)),
            *[dma((4, NCH)) for _ in range(8)],
            dma((3, 2 * OWN)), dma((3, OWN)),
        ],
        compiler_params=pltpu.CompilerParams(collective_id=0, has_side_effects=True, vmem_limit_bytes=VMEM),
        cost_estimate=pl.CostEstimate(flops=6 * TOK * D * D, transcendentals=0, bytes_accessed=64 * 2**20),
        name="project",
    )(x, gain, cos, sin, wq, wk, wv, wo)


def _attend(qt_ref, k_ref, vt_ref, seen_ref, q_s, k_s, v_s, far_s, mix_s, top_s, part_s, lse_s, flse_s, seen_s, gap_s,
            in_sem, q_sem, qs_sem, qr_sem, ps_sem, pr_sem, ls_sem, lr_sem, slot_sem, to_sem):
    dp, s, core, s1, s2, _ = _places()
    beside, across = (dp, s1), (dp, s2)
    first_chip = s < 2
    e = SCALE * LOG2E
    _greet((beside, across))

    def remote(src, dst, send, recv, device):
        return pltpu.make_async_remote_copy(src_ref=src, dst_ref=dst, send_sem=send, recv_sem=recv, device_id=device, device_id_type=MESH)

    def cols(t):
        return pl.ds(pl.multiple_of(t * STRIP, STRIP), STRIP)

    def place(p):
        return jnp.where(p < NS // 2, (1 - core) * (NS // 2) + NS // 2 - 1 - p, core * (NS // 2) + NS - 1 - p)

    def ask(t):
        return remote(qt_ref.at[:, :, cols(t)], far_s.at[:, :, cols(t)], qs_sem.at[t], qr_sem.at[t], across)

    def answer(t):
        slot = lax.rem(t, 2)
        return (remote(part_s.at[slot], far_s.at[:, :, cols(t)], ps_sem.at[slot], pr_sem.at[t], across),
                remote(lse_s.at[slot], flse_s.at[t], ls_sem.at[slot], lr_sem.at[t], across))

    def q_in(p):
        slot = lax.rem(p, 2)
        return pltpu.make_async_copy(qt_ref.at[:, :, cols(place(p))], q_s.at[slot], q_sem.at[slot])

    def sent(p):
        t, slot = place(p), lax.rem(p, 2)
        at = pl.ds(pl.multiple_of(lax.rem(t, NS // 2) * STRIP, STRIP), STRIP)
        return remote(seen_s.at[slot], seen_ref.at[pl.ds(core * OWN, OWN), at], slot_sem.at[slot], to_sem.at[lax.rem(t, NS // 2)], beside)

    def kept(p):
        t, slot = place(p), lax.rem(p, 2)
        at = pl.ds(pl.multiple_of(lax.rem(t, NS // 2) * STRIP, STRIP), STRIP)
        return pltpu.make_async_copy(seen_s.at[slot], seen_ref.at[pl.ds(core * OWN, OWN), at], slot_sem.at[slot])

    def hand(p):
        @pl.when(p < NS // 2)
        def _():
            sent(p).start()

        @pl.when(p >= NS // 2)
        def _():
            kept(p).start()

    def handed(p):
        @pl.when(p < NS // 2)
        def _():
            sent(p).wait_send()

        @pl.when(p >= NS // 2)
        def _():
            kept(p).wait()

    keys = pltpu.make_async_copy(k_ref, k_s, in_sem.at[0])
    values = pltpu.make_async_copy(vt_ref, v_s, in_sem.at[1])
    keys.start()
    values.start()
    q_in(0).start()

    @pl.when(jnp.logical_not(first_chip))
    def _():
        for t in range(NS):
            ask(t).start()

    gap_s[...] = lax.broadcasted_iota(jnp.int32, (STRIP, STRIP), 1) - lax.broadcasted_iota(jnp.int32, (STRIP, STRIP), 0)
    keys.wait()
    values.wait()
    ones = jnp.ones((8, STRIP), BF16)

    def block(j, t, query, masked):
        kj = cols(j)
        scores = [_dot(k_s[i, kj, :], query(i)) for i in range(OWN)]
        weights, keeps = [], []
        for i, sc in enumerate(scores):
            if masked:
                sc = jnp.where(gap_s[...] >= 0, sc, HIDDEN)
            old = top_s[i : i + 1, cols(t)]
            top = jnp.maximum(old, sc.max(axis=0, keepdims=True))
            top_s[i : i + 1, cols(t)] = top
            weights.append(jnp.exp2((sc - top) * e).astype(BF16))
            keeps.append(jnp.exp2((old - top) * e))
        for i in range(OWN):
            val = jnp.concatenate([v_s[i, :, kj], ones], axis=0)
            mix_s[i, :, cols(t)] = mix_s[i, :, cols(t)] * keeps[i] + _dot(val, weights[i])

    def clear(t):
        for i in range(OWN):
            top_s[i : i + 1, cols(t)] = jnp.full((1, STRIP), NEG, F32)
            mix_s[i, :, cols(t)] = jnp.zeros((HEAD + 8, STRIP), F32)

    def own(p):
        t, slot = place(p), lax.rem(p, 2)

        @pl.when(p + 1 < NS)
        def _():
            q_in(p + 1).start()

        q_in(p).wait()
        clear(t)
        lax.fori_loop(0, t, lambda j, _: block(j, t, lambda i: q_s[slot, i], False), None)
        block(t, t, lambda i: q_s[slot, i], True)

    def cross(p):
        ask(p).wait_recv()
        slot = lax.rem(p, 2)
        clear(p)
        lax.fori_loop(0, NS, lambda j, _: block(j, p, lambda i: far_s[i, :, cols(p)], False), None)

        @pl.when(p >= 2)
        def _():
            for c in answer(p - 2):
                c.wait_send()

        for i in range(OWN):
            total = mix_s[i, HEAD : HEAD + 1, cols(p)]
            part_s[slot, i] = (mix_s[i, :HEAD, cols(p)] * (1 / total)).astype(BF16)
            lse_s[slot, i : i + 1, :] = top_s[i : i + 1, cols(p)] * SCALE + jnp.log(total)
        for c in answer(p):
            c.start()

    def finish(p):
        t, slot = place(p), lax.rem(p, 2)

        @pl.when(p >= 2)
        def _():
            handed(p - 2)

        for i in range(OWN):
            total = mix_s[i, HEAD : HEAD + 1, cols(t)]
            seen_s[slot, i] = (mix_s[i, :HEAD, cols(t)] * (1 / total)).T.astype(BF16)
        hand(p)

    def join(p, t):
        slot = lax.rem(p, 2)

        @pl.when(p >= 2)
        def _():
            handed(p - 2)

        for i in range(OWN):
            total = mix_s[i, HEAD : HEAD + 1, cols(t)]
            mine = top_s[i : i + 1, cols(t)] * SCALE + jnp.log(total)
            theirs = flse_s[t, i : i + 1, :]
            top = jnp.maximum(mine, theirs)
            wm, wt = jnp.exp(mine - top), jnp.exp(theirs - top)
            both = 1 / (wm + wt)
            mixed = mix_s[i, :HEAD, cols(t)] * (wm * both / total) + far_s[i, :, cols(t)].astype(F32) * (wt * both)
            seen_s[slot, i] = mixed.T.astype(BF16)
        hand(p)

    def step(p, _):
        own(p)

        @pl.when(first_chip)
        def _():
            finish(p)
            cross(p)

    lax.fori_loop(0, NS, step, None)

    @pl.when(first_chip)
    def _():
        for p in (NS - 2, NS - 1):
            for c in answer(p):
                c.wait_send()

    @pl.when(jnp.logical_not(first_chip))
    def _():
        for t in range(NS):
            ask(t).wait_send()

        def merge(p, _):
            t = place(p)
            for c in answer(t):
                c.wait_recv()
            join(p, t)

        lax.fori_loop(0, NS, merge, None)

    handed(NS - 2)
    handed(NS - 1)
    for p in range(NS // 2):
        sent(p).wait_recv()


def attend(qt, k, vt):
    hbm = pl.BlockSpec(memory_space=pltpu.HBM)
    dma = pltpu.SemaphoreType.DMA
    return pl.pallas_call(
        _attend,
        in_specs=[hbm] * 3,
        out_specs=hbm,
        out_shape=jax.ShapeDtypeStruct((HEADS, TOK, HEAD), BF16),
        scratch_shapes=[
            pltpu.VMEM((2, OWN, HEAD, STRIP), BF16),
            pltpu.VMEM((OWN, CHIP, HEAD), BF16),
            pltpu.VMEM((OWN, HEAD, CHIP), BF16),
            pltpu.VMEM((OWN, HEAD, CHIP), BF16),
            pltpu.VMEM((OWN, HEAD + 8, CHIP), F32),
            pltpu.VMEM((OWN, CHIP), F32),
            pltpu.VMEM((2, OWN, HEAD, STRIP), BF16),
            pltpu.VMEM((2, OWN, STRIP), F32),
            pltpu.VMEM((NS, OWN, STRIP), F32),
            pltpu.VMEM((2, OWN, STRIP, HEAD), BF16),
            pltpu.VMEM((STRIP, STRIP), jnp.int32),
            dma((2,)), dma((2,)), dma((NS,)), dma((NS,)), dma((2,)), dma((NS,)), dma((2,)), dma((NS,)), dma((2,)), dma((NS // 2,)),
        ],
        compiler_params=pltpu.CompilerParams(collective_id=1, has_side_effects=True, vmem_limit_bytes=VMEM),
        cost_estimate=pl.CostEstimate(flops=6 * OWN * CHIP * CHIP * HEAD, transcendentals=OWN * CHIP * CHIP, bytes_accessed=64 * 2**20),
        name="attend",
    )(qt, k, vt)


def _output(place_ref, seen_ref, x_ref, wo_ref, rest_ref, y_ref):
    s = place_ref[0]
    lhs = jnp.concatenate([seen_ref[place_ref[j] * 2 + i] for j in range(4) for i in range(2)], axis=1)

    def part(n, _):
        at = pl.ds(pl.multiple_of(n * 512, 512), 512)
        w = jnp.concatenate([wo_ref[:, at], rest_ref[:, at]], axis=0)
        y_ref[:, at] = (x_ref[:, at].astype(F32) + _dot(lhs, w)).astype(BF16)

    lax.fori_loop(0, D // 512, part, None)


def output(seen, x, wo, rest, place):
    rows = 512
    return pl.pallas_call(
        _output,
        grid_spec=pltpu.PrefetchScalarGridSpec(
            num_scalar_prefetch=1,
            grid=(TOK // rows,),
            in_specs=[
                pl.BlockSpec((HEADS, rows, HEAD), lambda i, _: (0, i, 0)),
                pl.BlockSpec((rows, D), lambda i, _: (i, 0)),
                pl.BlockSpec((PIECE, D), lambda i, _: (0, 0)),
                pl.BlockSpec((3 * PIECE, D), lambda i, _: (0, 0)),
            ],
            out_specs=pl.BlockSpec((rows, D), lambda i, _: (i, 0)),
        ),
        out_shape=jax.ShapeDtypeStruct((TOK, D), BF16),
        compiler_params=pltpu.CompilerParams(dimension_semantics=("arbitrary",), vmem_limit_bytes=56 * 2**20),
        cost_estimate=pl.CostEstimate(flops=2 * TOK * D * D, transcendentals=0, bytes_accessed=32 * 2**20),
        name="output",
    )(place, seen, x, wo, rest)


def solution(mesh):
    def step(x, gain, wq, wk, wv, wo):
        s = lax.axis_index("sp")
        place = s * TOK + jnp.arange(TOK)
        half = HEAD // 2
        angle = place.astype(F32)[:, None] * THETA ** (-jnp.arange(half, dtype=F32) / half)
        qt, k, vt, rest = project(x, gain[None], jnp.cos(angle), jnp.sin(angle), wq, wk, wv, wo)
        seen = attend(qt, k, vt)
        s1 = s + 1 - 2 * lax.rem(s, 2)
        order = jnp.stack([s, s1, lax.rem(s + 2, 4), lax.rem(s1 + 2, 4)]).astype(jnp.int32)
        return output(seen, x, wo, rest, order)

    tokens, whole = P(("dp", "sp"), None), P("sp", None)
    return jax.shard_map(
        step,
        mesh=mesh,
        in_specs=(tokens, P(None), whole, whole, whole, whole),
        out_specs=tokens,
        check_vma=False,
    )
```

```python
import functools

import jax
import jax.numpy as jnp
from jax import lax
from jax.experimental import pallas as pl
from jax.experimental.pallas import tpu as pltpu
from jax.sharding import PartitionSpec as P

NEG = -1e30
HIDDEN = 2 * NEG
LOG2E = 1.4426950408889634
HEAD = 256
HEADS = 8
OWN = 4
D = 2048
TOK = 2048
CHIP = 2 * TOK
PIECE = D // 4
HALF = PIECE // 2
NCH = 4
CH = HALF // NCH
STRIP = 512
NS = CHIP // STRIP
THETA = 10000
EARLY = 1
FINE = 64
SCALE = HEAD**-0.5
MESH = pl.DeviceIdType.MESH
VMEM = 63 * 2**20
F32, BF16 = jnp.float32, jnp.bfloat16


def _places():
    dp, s = lax.axis_index("dp"), lax.axis_index("sp")
    core = lax.rem(s, 2)
    s1 = s + 1 - 2 * core
    s2, s3 = lax.rem(s + 2, 4), lax.rem(s1 + 2, 4)
    return dp, s, core, s1, s2, s3


def _greet(devices):
    barrier = pltpu.get_barrier_semaphore()
    for d in devices:
        pl.semaphore_signal(barrier, inc=1, device_id=d, device_id_type=MESH)
    pl.semaphore_wait(barrier, len(devices))


def _remote(src, dst, send, recv, device):
    return pltpu.make_async_remote_copy(src_ref=src, dst_ref=dst, send_sem=send, recv_sem=recv, device_id=device, device_id_type=MESH)


def _dot(a, b):
    return jnp.dot(a, b, preferred_element_type=F32)


class _Gather:
    def __init__(self, w_ref, held, sems, m):
        dp, s, core, s1, s2, s3 = _places()
        own_send, own_recv, x_send, x_recv, y_send, y_recv, d_send, d_recv, e_send, e_recv = sems
        beside, across, other = (dp, s1), (dp, s2), (1 - dp, s)
        mine, theirs = dp * HALF, (1 - dp) * HALF

        def own(n=None):
            return _remote(w_ref, held(PIECE, PIECE), own_send.at[m], own_recv.at[m], beside)

        def x(n):
            return _remote(w_ref.at[pl.ds(mine + n * CH, CH)], held(2 * PIECE + mine + n * CH, CH), x_send.at[m, n], x_recv.at[m, n], across)

        def y(n):
            at = 2 * PIECE + mine + n * CH
            return _remote(held(at, CH), held(at, CH), y_send.at[m, n], y_recv.at[m, n], other)

        def d(n):
            at = 2 * PIECE + mine + n * CH
            return _remote(held(at, CH), held(PIECE + at, CH), d_send.at[m, n], d_recv.at[m, n], beside)

        def e(n):
            at = 2 * PIECE + theirs + n * CH
            return _remote(held(at, CH), held(PIECE + at, CH), e_send.at[m, n], e_recv.at[m, n], beside)

        self.own, self.x, self.y, self.d, self.e = own, x, y, d, e

    def start_x(self):
        for n in range(NCH):
            self.x(n).start()

    def pass_x(self, n):
        self.x(n).wait_recv()
        self.y(n).start()
        self.d(n).start()

    def pass_y(self, n):
        self.y(n).wait_recv()
        self.e(n).start()

    def arrived(self):
        for n in range(NCH):
            self.d(n).wait_recv()
            self.e(n).wait_recv()

    def left(self):
        self.own().wait_send()
        for n in range(NCH):
            self.x(n).wait_send()
        self.passed()

    def passed(self):
        for n in range(NCH):
            for c in (self.y, self.d, self.e):
                c(n).wait_send()


def _gather_sems(count):
    dma = pltpu.SemaphoreType.DMA
    return [dma((count,)), dma((count,))] + [dma((count, NCH)) for _ in range(8)]


def _early(core, p):
    return lax.rem(core * (NS // 2) + p, NS)


def _cols(t):
    return pl.ds(pl.multiple_of(t * STRIP, STRIP), STRIP)


def _project(x_ref, gain_ref, far_ref, near_ref, wq_ref, wk_ref, wv_ref, wo_ref, qt_ref, k_ref, vt_ref, ask_ref, rest_ref,
             a_s, x_s, w_s, p_s, t_s, k_s, cos_s, sin_s, x_sem, l_sem, slot_sem, to_sem, as_sem, ar_sem, *g_sem):
    dp, s, core, s1, s2, s3 = _places()
    beside, across, other = (dp, s1), (dp, s2), (1 - dp, s)
    first_chip = s < 2
    w_refs = (wq_ref, wk_ref, wv_ref)
    _greet((beside, across, other))
    gathers = [_Gather(w_refs[m], lambda row, n, m=m: w_s.at[m, pl.ds(row, n)], g_sem, m) for m in range(3)]
    wo = _Gather(wo_ref, lambda row, n: rest_ref.at[pl.ds(row - PIECE, n)], g_sem, 3)

    def local_copy(m):
        return pltpu.make_async_copy(w_refs[m], w_s.at[m, pl.ds(0, PIECE)], l_sem.at[m])

    XR = x_s.shape[1]
    steps = TOK // XR

    def x_in(n):
        return pltpu.make_async_copy(x_ref.at[pl.ds(n * XR, XR)], x_s.at[lax.rem(n, 2)], x_sem.at[lax.rem(n, 2)])

    x_in(0).start()
    for m in range(3):
        gathers[m].start_x()
    pl.when(first_chip)(wo.start_x)
    for m in range(3):
        gathers[m].own().start()
        local_copy(m).start()
    wo.own().start()

    def norm(n, _):
        @pl.when(n + 1 < steps)
        def _():
            x_in(n + 1).start()

        x_in(n).wait()
        slot = lax.rem(n, 2)
        wide = x_s[slot].astype(F32)
        scale = lax.rsqrt(jnp.mean(wide * wide, -1, keepdims=True) + 1e-6)
        for j, p in enumerate((s, s1, s2, s3)):
            cols = pl.ds(pl.multiple_of(p * PIECE, PIECE), PIECE)
            a = x_s[slot, :, cols].astype(F32) * scale * gain_ref[:, cols].astype(F32)
            a_s[pl.ds(pl.multiple_of(n * XR, XR), XR), j * PIECE : (j + 1) * PIECE] = a.astype(BF16)

    lax.fori_loop(0, steps, norm, None)

    def head_cols(h):
        return pl.ds(pl.multiple_of(h * HEAD, HEAD), HEAD)

    gathers[0].own().wait_recv()
    local_copy(0).wait()

    def begin(n, _):
        gathers[0].pass_x(n)
        for h in range(2):
            cols = head_cols(2 * n + h)

            def strip(r, _):
                p_s[_cols(r), cols] = _dot(a_s[_cols(r), : 2 * PIECE], w_s[0, : 2 * PIECE, cols])

            lax.fori_loop(0, TOK // STRIP, strip, None)

    lax.fori_loop(0, NCH, begin, None)

    def table(n, _):
        at = pl.ds(pl.multiple_of(n * FINE, FINE), FINE)
        fc, fs = far_ref[0, pl.ds(n, 1), :], far_ref[1, pl.ds(n, 1), :]
        cos_s[at, :] = fc * near_ref[0] - fs * near_ref[1]
        sin_s[at, :] = fs * near_ref[0] + fc * near_ref[1]

    lax.fori_loop(0, TOK // FINE, table, None)
    for n in range(NCH):
        gathers[0].pass_y(n)

    outs = (qt_ref, k_ref, vt_ref)
    here = pl.ds(pl.multiple_of(core * TOK, TOK), TOK)

    def stage(m):
        return k_s if m == 1 else t_s

    def out(m, n):
        return outs[m].at[n, here, :] if m == 1 else outs[m].at[n, :, here]

    def sent(m, n):
        slot = lax.rem(n, 2)
        return _remote(stage(m).at[slot], out(m, n), slot_sem.at[0, slot], to_sem.at[m, n], beside)

    def kept(m, n):
        slot = lax.rem(n, 2)
        return pltpu.make_async_copy(stage(m).at[2 + slot], out(m, n), slot_sem.at[1, slot])

    def ask(p):
        return _remote(qt_ref.at[:, :, _cols(_early(core, p))], ask_ref.at[p], as_sem.at[p], ar_sem.at[p], across)

    def make(m, h, slot):
        cols = head_cols(h)

        def strip(r, _):
            rows = _cols(r)
            if m == 0:
                t = p_s[rows, cols] + _dot(a_s[rows, 2 * PIECE :], w_s[m, 2 * PIECE :, cols])
            else:
                t = _dot(a_s[rows, :], w_s[m, :, cols])
            t = t.astype(BF16)
            if m < 2:
                t = t.astype(F32)
                lo, hi = t[:, : HEAD // 2], t[:, HEAD // 2 :]
                cos, sin = cos_s[rows, :], sin_s[rows, :]
                t = jnp.concatenate([lo * cos - hi * sin, hi * cos + lo * sin], axis=1).astype(BF16)
            if m == 1:
                k_s[slot, rows, :] = t
            else:
                t_s[slot, :, rows] = t.T

        lax.fori_loop(0, TOK // STRIP, strip, None)

    for m in range(3):
        gathers[m].arrived()
        if m:
            gathers[m].own().wait_recv()
            local_copy(m).wait()

        def away(n, _):
            @pl.when(n >= 2)
            def _():
                sent(m, n - 2).wait_send()

            make(m, (1 - core) * OWN + n, lax.rem(n, 2))
            sent(m, n).start()
            if m < 2:
                gathers[m + 1].pass_x(n)
            else:
                pl.when(jnp.logical_not(first_chip))(lambda: wo.pass_x(n))

        def home(n, _):
            @pl.when(n >= 2)
            def _():
                kept(m, n - 2).wait()

            if m < 2:
                gathers[m + 1].pass_y(n)
            else:
                pl.when(jnp.logical_not(first_chip))(lambda: wo.pass_y(n))
            make(m, core * OWN + n, 2 + lax.rem(n, 2))
            kept(m, n).start()

        lax.fori_loop(0, OWN, away, None)
        lax.fori_loop(0, OWN, home, None)
        for n in (OWN - 2, OWN - 1):
            sent(m, n).wait_send()
            kept(m, n).wait()
        if m == 0:

            @pl.when(jnp.logical_not(first_chip))
            def _():
                for p in range(EARLY):
                    ask(p).start()

    for g in gathers:
        g.left()
    wo.own().wait_recv()
    wo.own().wait_send()
    for m in range(3):
        for n in range(OWN):
            sent(m, n).wait_recv()

    @pl.when(first_chip)
    def _():
        for n in range(NCH):
            wo.x(n).wait_send()
        for p in range(EARLY):
            ask(p).wait_recv()

    @pl.when(jnp.logical_not(first_chip))
    def _():
        wo.arrived()
        wo.passed()
        for p in range(EARLY):
            ask(p).wait_send()


def project(x, gain, far, near, wq, wk, wv, wo):
    hbm, vmem = pl.BlockSpec(memory_space=pltpu.HBM), pl.BlockSpec(memory_space=pltpu.VMEM)
    dma = pltpu.SemaphoreType.DMA
    return pl.pallas_call(
        _project,
        in_specs=[hbm, vmem, vmem, vmem, hbm, hbm, hbm, hbm],
        out_specs=[hbm] * 5,
        out_shape=[
            jax.ShapeDtypeStruct((OWN, HEAD, CHIP), BF16),
            jax.ShapeDtypeStruct((OWN, CHIP, HEAD), BF16),
            jax.ShapeDtypeStruct((OWN, HEAD, CHIP), BF16),
            jax.ShapeDtypeStruct((EARLY, OWN, HEAD, STRIP), BF16),
            jax.ShapeDtypeStruct((3 * PIECE, D), BF16),
        ],
        scratch_shapes=[
            pltpu.VMEM((TOK, D), BF16),
            pltpu.VMEM((2, 256, D), BF16),
            pltpu.VMEM((3, D, D), BF16),
            pltpu.VMEM((TOK, D), F32),
            pltpu.VMEM((4, HEAD, TOK), BF16),
            pltpu.VMEM((4, TOK, HEAD), BF16),
            pltpu.VMEM((TOK, HEAD // 2), F32),
            pltpu.VMEM((TOK, HEAD // 2), F32),
            dma((2,)), dma((3,)), dma((2, 2)), dma((3, OWN)), dma((EARLY,)), dma((EARLY,)),
            *_gather_sems(4),
        ],
        compiler_params=pltpu.CompilerParams(collective_id=0, has_side_effects=True, vmem_limit_bytes=VMEM),
        cost_estimate=pl.CostEstimate(flops=6 * TOK * D * D, transcendentals=0, bytes_accessed=64 * 2**20),
        name="project",
    )(x, gain, far, near, wq, wk, wv, wo)


def _attend(qt_ref, k_ref, vt_ref, ask_ref, wo_ref, _, seen_ref, rest_ref,
            q_s, k_s, v_s, far_s, mix_s, top_s, part_s, lse_s, flse_s, seen_s, sa_s, sb_s,
            in_sem, q_sem, f_sem, qs_sem, qr_sem, ps_sem, pr_sem, ls_sem, lr_sem, slot_sem, to_sem, *g_sem):
    dp, s, core, s1, s2, _ = _places()
    beside, across, other = (dp, s1), (dp, s2), (1 - dp, s)
    first_chip = s < 2
    e = SCALE * LOG2E
    _greet((beside, across, other))
    wo = _Gather(wo_ref, lambda row, n: rest_ref.at[pl.ds(row - PIECE, n)], g_sem, 0)
    cols = _cols

    def early(p):
        return _early(core, p)

    def place(p):
        return jnp.where(p < NS // 2, (1 - core) * (NS // 2) + NS // 2 - 1 - p, core * (NS // 2) + NS - 1 - p)

    def ask(p):
        at = cols(early(p))
        return _remote(qt_ref.at[:, :, at], far_s.at[:, :, at], qs_sem.at[p], qr_sem.at[p], across)

    def asked(p):
        return pltpu.make_async_copy(ask_ref.at[p], far_s.at[:, :, cols(early(p))], f_sem.at[p])

    def answer(p):
        slot = lax.rem(p, 2)
        return (_remote(part_s.at[slot], far_s.at[:, :, cols(early(p))], ps_sem.at[slot], pr_sem.at[p], across),
                _remote(lse_s.at[slot], flse_s.at[p], ls_sem.at[slot], lr_sem.at[p], across))

    def q_in(p):
        slot = lax.rem(p, 2)
        return pltpu.make_async_copy(qt_ref.at[:, :, cols(place(p))], q_s.at[slot], q_sem.at[slot])

    def ours(t):
        return lax.div(t, NS // 2) == core

    def target(t):
        return seen_ref.at[pl.ds(core * OWN, OWN), cols(lax.rem(t, NS // 2))]

    def sent(t, slot):
        return _remote(seen_s.at[slot], target(t), slot_sem.at[slot], to_sem.at[lax.rem(t, NS // 2)], beside)

    def kept(t, slot):
        return pltpu.make_async_copy(seen_s.at[slot], target(t), slot_sem.at[slot])

    def hand(t, slot):
        @pl.when(ours(t))
        def _():
            kept(t, slot).start()

        @pl.when(jnp.logical_not(ours(t)))
        def _():
            sent(t, slot).start()

    def handed(t, slot):
        @pl.when(ours(t))
        def _():
            kept(t, slot).wait()

        @pl.when(jnp.logical_not(ours(t)))
        def _():
            sent(t, slot).wait_send()

    keys = pltpu.make_async_copy(k_ref, k_s, in_sem.at[0])
    values = pltpu.make_async_copy(vt_ref, v_s, in_sem.at[1])
    q_in(0).start()
    keys.start()
    values.start()

    @pl.when(jnp.logical_not(first_chip))
    def _():
        for p in range(EARLY, NS):
            ask(p).start()
        wo.start_x()

    @pl.when(first_chip)
    def _():
        for p in range(EARLY):
            asked(p).start()

    keys.wait()
    values.wait()
    ones = jnp.ones((8, STRIP), BF16)

    def clear(t):
        for i in range(OWN):
            top_s[i : i + 1, cols(t)] = jnp.full((1, STRIP), NEG, F32)
            mix_s[i, :, cols(t)] = jnp.zeros((HEAD + 8, STRIP), F32)

    def run(t, query, masked, count):
        def score(i, j, into):
            into[i] = _dot(k_s[i, cols(j), :], query(i))

        def fold(i, j, held, cut):
            sc = held[i]
            if cut:
                query_at, key_at = (lax.broadcasted_iota(jnp.int32, (STRIP, STRIP), n) for n in (1, 0))
                sc = jnp.where(query_at >= key_at, sc, HIDDEN)
            old = top_s[i : i + 1, cols(t)]
            top = jnp.maximum(old, sc.max(axis=0, keepdims=True))
            top_s[i : i + 1, cols(t)] = top
            weights = jnp.exp2((sc - top) * e).astype(BF16)
            keep = jnp.exp2((old - top) * e)
            val = jnp.concatenate([v_s[i, :, cols(j)], ones], axis=0)
            mix_s[i, :, cols(t)] = mix_s[i, :, cols(t)] * keep + _dot(val, weights)

        def step(j, held, after, into, cut=False):
            for i in range(OWN):
                if after is not None:
                    score(i, after, into)
                fold(i, j, held, cut)

        def pair(n, _):
            step(2 * n, sa_s, 2 * n + 1, sb_s)
            step(2 * n + 1, sb_s, 2 * n + 2, sa_s)

        def single():
            step(count - 1, sa_s, None, None)

        def double():
            step(count - 2, sa_s, count - 1, sb_s)
            step(count - 1, sb_s, None, None)

        clear(t)
        if masked:
            for i in range(OWN):
                score(i, t, sb_s)
            step(t, sb_s, 0, sa_s, True)
            lax.fori_loop(0, lax.div(jnp.maximum(count - 1, 0), 2), pair, None)
            pl.when(lax.rem(count, 2) == 1)(single)
            pl.when((lax.rem(count, 2) == 0) & (count > 0))(double)
        else:
            for i in range(OWN):
                score(i, 0, sa_s)
            lax.fori_loop(0, (count - 1) // 2, pair, None)
            double()

    def own(p):
        t, slot = place(p), lax.rem(p, 2)

        @pl.when(p + 1 < NS)
        def _():
            q_in(p + 1).start()

        q_in(p).wait()
        run(t, lambda i: q_s[slot, i], True, t)

    def cross(p):
        t = early(p)

        @pl.when(p < EARLY)
        def _():
            asked(p).wait()

        @pl.when(p >= EARLY)
        def _():
            ask(p).wait_recv()

        slot = lax.rem(p, 2)
        run(t, lambda i: far_s[i, :, cols(t)], False, NS)

        @pl.when(p >= 2)
        def _():
            for c in answer(p - 2):
                c.wait_send()

        for i in range(OWN):
            total = mix_s[i, HEAD : HEAD + 1, cols(t)]
            part_s[slot, i] = (mix_s[i, :HEAD, cols(t)] * (1 / total)).astype(BF16)
            lse_s[slot, i : i + 1, :] = top_s[i : i + 1, cols(t)] * SCALE + jnp.log(total)
        for c in answer(p):
            c.start()

    def finish(p):
        t, slot = place(p), lax.rem(p, 2)

        @pl.when(p >= 2)
        def _():
            handed(place(p - 2), slot)

        for i in range(OWN):
            total = mix_s[i, HEAD : HEAD + 1, cols(t)]
            seen_s[slot, i] = (mix_s[i, :HEAD, cols(t)] * (1 / total)).T.astype(BF16)
        hand(t, slot)

    def join(p):
        t, slot = early(p), lax.rem(p, 2)

        @pl.when(p >= 2)
        def _():
            handed(early(p - 2), slot)

        for i in range(OWN):
            total = mix_s[i, HEAD : HEAD + 1, cols(t)]
            mine = top_s[i : i + 1, cols(t)] * SCALE + jnp.log(total)
            theirs = flse_s[p, i : i + 1, :]
            top = jnp.maximum(mine, theirs)
            wm, wt = jnp.exp(mine - top), jnp.exp(theirs - top)
            both = 1 / (wm + wt)
            mixed = mix_s[i, :HEAD, cols(t)] * (wm * both / total) + far_s[i, :, cols(t)].astype(F32) * (wt * both)
            seen_s[slot, i] = mixed.T.astype(BF16)
        hand(t, slot)

    def step(p, _):
        @pl.when(first_chip)
        def _():
            cross(p)

        own(p)

        @pl.when(first_chip)
        def _():
            finish(p)

    lax.fori_loop(0, NS, step, None)

    @pl.when(first_chip)
    def _():
        for n in range(NCH):
            wo.pass_x(n)
        for n in range(NCH):
            wo.pass_y(n)
        for p in (NS - 2, NS - 1):
            for c in answer(p):
                c.wait_send()
            handed(place(p), p % 2)
        wo.arrived()
        wo.passed()

    @pl.when(jnp.logical_not(first_chip))
    def _():
        for p in range(EARLY, NS):
            ask(p).wait_send()
        for n in range(NCH):
            wo.x(n).wait_send()

        def merge(p, _):
            for c in answer(p):
                c.wait_recv()
            join(p)

        lax.fori_loop(0, NS, merge, None)
        for p in (NS - 2, NS - 1):
            handed(early(p), p % 2)

    for n in range(NS // 2):
        sent(n, 0).wait_recv()


def attend(qt, k, vt, asked, wo, rest):
    hbm = pl.BlockSpec(memory_space=pltpu.HBM)
    dma = pltpu.SemaphoreType.DMA
    return pl.pallas_call(
        _attend,
        in_specs=[hbm] * 6,
        out_specs=[hbm] * 2,
        input_output_aliases={5: 1},
        out_shape=[jax.ShapeDtypeStruct((HEADS, TOK, HEAD), BF16), jax.ShapeDtypeStruct((3 * PIECE, D), BF16)],
        scratch_shapes=[
            pltpu.VMEM((2, OWN, HEAD, STRIP), BF16),
            pltpu.VMEM((OWN, CHIP, HEAD), BF16),
            pltpu.VMEM((OWN, HEAD, CHIP), BF16),
            pltpu.VMEM((OWN, HEAD, CHIP), BF16),
            pltpu.VMEM((OWN, HEAD + 8, CHIP), F32),
            pltpu.VMEM((OWN, CHIP), F32),
            pltpu.VMEM((2, OWN, HEAD, STRIP), BF16),
            pltpu.VMEM((2, OWN, STRIP), F32),
            pltpu.VMEM((NS, OWN, STRIP), F32),
            pltpu.VMEM((2, OWN, STRIP, HEAD), BF16),
            pltpu.VMEM((OWN, STRIP, STRIP), F32),
            pltpu.VMEM((OWN, STRIP, STRIP), F32),
            dma((2,)), dma((2,)), dma((EARLY,)), dma((NS,)), dma((NS,)), dma((2,)), dma((NS,)), dma((2,)), dma((NS,)), dma((2,)),
            dma((NS // 2,)),
            *_gather_sems(1),
        ],
        compiler_params=pltpu.CompilerParams(collective_id=1, has_side_effects=True, vmem_limit_bytes=VMEM),
        cost_estimate=pl.CostEstimate(flops=6 * OWN * CHIP * CHIP * HEAD, transcendentals=OWN * CHIP * CHIP, bytes_accessed=64 * 2**20),
        name="attend",
    )(qt, k, vt, asked, wo, rest)


def _output(place_ref, seen_ref, x_ref, wo_ref, rest_ref, y_ref):
    s = place_ref[0]
    lhs = jnp.concatenate([seen_ref[place_ref[j] * 2 + i] for j in range(4) for i in range(2)], axis=1)

    def part(n, _):
        at = pl.ds(pl.multiple_of(n * 512, 512), 512)
        w = jnp.concatenate([wo_ref[:, at], rest_ref[:, at]], axis=0)
        y_ref[:, at] = (x_ref[:, at].astype(F32) + _dot(lhs, w)).astype(BF16)

    lax.fori_loop(0, D // 512, part, None)


def output(seen, x, wo, rest, place):
    rows = 512
    return pl.pallas_call(
        _output,
        grid_spec=pltpu.PrefetchScalarGridSpec(
            num_scalar_prefetch=1,
            grid=(TOK // rows,),
            in_specs=[
                pl.BlockSpec((HEADS, rows, HEAD), lambda i, _: (0, i, 0)),
                pl.BlockSpec((rows, D), lambda i, _: (i, 0)),
                pl.BlockSpec((PIECE, D), lambda i, _: (0, 0)),
                pl.BlockSpec((3 * PIECE, D), lambda i, _: (0, 0)),
            ],
            out_specs=pl.BlockSpec((rows, D), lambda i, _: (i, 0)),
        ),
        out_shape=jax.ShapeDtypeStruct((TOK, D), BF16),
        compiler_params=pltpu.CompilerParams(dimension_semantics=("arbitrary",), vmem_limit_bytes=56 * 2**20),
        cost_estimate=pl.CostEstimate(flops=2 * TOK * D * D, transcendentals=0, bytes_accessed=32 * 2**20),
        name="output",
    )(place, seen, x, wo, rest)


def solution(mesh):
    def step(x, gain, wq, wk, wv, wo):
        s = lax.axis_index("sp")
        rate = THETA ** (-jnp.arange(HEAD // 2, dtype=F32) / (HEAD // 2))

        def table(place):
            angle = place.astype(F32)[:, None] * rate
            return jnp.stack([jnp.cos(angle), jnp.sin(angle)])

        far, near = table(s * TOK + FINE * jnp.arange(TOK // FINE)), table(jnp.arange(FINE))
        qt, k, vt, asked, rest = project(x, gain[None], far, near, wq, wk, wv, wo)
        seen, rest = attend(qt, k, vt, asked, wo, rest)
        s1 = s + 1 - 2 * lax.rem(s, 2)
        order = jnp.stack([s, s1, lax.rem(s + 2, 4), lax.rem(s1 + 2, 4)]).astype(jnp.int32)
        return output(seen, x, wo, rest, order)

    tokens, whole = P(("dp", "sp"), None), P("sp", None)
    return jax.shard_map(
        step,
        mesh=mesh,
        in_specs=(tokens, P(None), whole, whole, whole, whole),
        out_specs=tokens,
        check_vma=False,
    )
```

```python
import functools

import jax
import jax.numpy as jnp
from jax import lax
from jax.experimental import pallas as pl
from jax.experimental.pallas import tpu as pltpu
from jax.sharding import PartitionSpec as P

NEG = -1e30
HIDDEN = 2 * NEG
LOG2E = 1.4426950408889634
HEAD = 256
HEADS = 8
OWN = 4
D = 2048
TOK = 2048
CHIP = 2 * TOK
PIECE = D // 4
HALF = PIECE // 2
NCH = 4
CH = HALF // NCH
STRIP = 512
NS = CHIP // STRIP
THETA = 10000
EARLY = 1
FINE = 64
SCALE = HEAD**-0.5
MESH = pl.DeviceIdType.MESH
VMEM = 63 * 2**20
F32, BF16 = jnp.float32, jnp.bfloat16


def _places():
    dp, s = lax.axis_index("dp"), lax.axis_index("sp")
    core = lax.rem(s, 2)
    s1 = s + 1 - 2 * core
    s2, s3 = lax.rem(s + 2, 4), lax.rem(s1 + 2, 4)
    return dp, s, core, s1, s2, s3


def _greet(devices):
    barrier = pltpu.get_barrier_semaphore()
    for d in devices:
        pl.semaphore_signal(barrier, inc=1, device_id=d, device_id_type=MESH)
    pl.semaphore_wait(barrier, len(devices))


def _remote(src, dst, send, recv, device):
    return pltpu.make_async_remote_copy(src_ref=src, dst_ref=dst, send_sem=send, recv_sem=recv, device_id=device, device_id_type=MESH)


def _dot(a, b):
    return jnp.dot(a, b, preferred_element_type=F32)


class _Gather:
    def __init__(self, w_ref, held, sems, m):
        dp, s, core, s1, s2, s3 = _places()
        own_send, own_recv, x_send, x_recv, y_send, y_recv, d_send, d_recv, e_send, e_recv = sems
        beside, across, other = (dp, s1), (dp, s2), (1 - dp, s)
        mine, theirs = dp * HALF, (1 - dp) * HALF

        def own(n=None):
            return _remote(w_ref, held(PIECE, PIECE), own_send.at[m], own_recv.at[m], beside)

        def x(n):
            return _remote(w_ref.at[pl.ds(mine + n * CH, CH)], held(2 * PIECE + mine + n * CH, CH), x_send.at[m, n], x_recv.at[m, n], across)

        def y(n):
            at = 2 * PIECE + mine + n * CH
            return _remote(held(at, CH), held(at, CH), y_send.at[m, n], y_recv.at[m, n], other)

        def d(n):
            at = 2 * PIECE + mine + n * CH
            return _remote(held(at, CH), held(PIECE + at, CH), d_send.at[m, n], d_recv.at[m, n], beside)

        def e(n):
            at = 2 * PIECE + theirs + n * CH
            return _remote(held(at, CH), held(PIECE + at, CH), e_send.at[m, n], e_recv.at[m, n], beside)

        self.own, self.x, self.y, self.d, self.e = own, x, y, d, e

    def start_x(self):
        for n in range(NCH):
            self.x(n).start()

    def pass_x(self, n):
        self.x(n).wait_recv()
        self.y(n).start()
        self.d(n).start()

    def pass_y(self, n):
        self.y(n).wait_recv()
        self.e(n).start()

    def arrived(self):
        for n in range(NCH):
            self.d(n).wait_recv()
            self.e(n).wait_recv()

    def left(self):
        self.own().wait_send()
        for n in range(NCH):
            self.x(n).wait_send()
        self.passed()

    def passed(self):
        for n in range(NCH):
            for c in (self.y, self.d, self.e):
                c(n).wait_send()


def _gather_sems(count):
    dma = pltpu.SemaphoreType.DMA
    return [dma((count,)), dma((count,))] + [dma((count, NCH)) for _ in range(8)]


def _early(core, p):
    return lax.rem(core * (NS // 2) + p, NS)


def _cols(t):
    return pl.ds(pl.multiple_of(t * STRIP, STRIP), STRIP)


def _project(x_ref, gain_ref, far_ref, near_ref, wq_ref, wk_ref, wv_ref, qt_ref, k_ref, vt_ref, ask_ref,
             a_s, x_s, w_s, p_s, t_s, k_s, cos_s, sin_s, x_sem, l_sem, slot_sem, to_sem, as_sem, ar_sem, *g_sem):
    dp, s, core, s1, s2, s3 = _places()
    beside, across, other = (dp, s1), (dp, s2), (1 - dp, s)
    first_chip = s < 2
    w_refs = (wq_ref, wk_ref, wv_ref)
    _greet((beside, across, other))
    gathers = [_Gather(w_refs[m], lambda row, n, m=m: w_s.at[m, pl.ds(row, n)], g_sem, m) for m in range(3)]

    def local_copy(m):
        return pltpu.make_async_copy(w_refs[m], w_s.at[m, pl.ds(0, PIECE)], l_sem.at[m])

    XR = x_s.shape[1]
    steps = TOK // XR

    def x_in(n):
        return pltpu.make_async_copy(x_ref.at[pl.ds(n * XR, XR)], x_s.at[lax.rem(n, 2)], x_sem.at[lax.rem(n, 2)])

    x_in(0).start()
    for m in range(3):
        gathers[m].start_x()
    for m in range(3):
        gathers[m].own().start()
        local_copy(m).start()

    def norm(n, _):
        @pl.when(n + 1 < steps)
        def _():
            x_in(n + 1).start()

        x_in(n).wait()
        slot = lax.rem(n, 2)
        wide = x_s[slot].astype(F32)
        scale = lax.rsqrt(jnp.mean(wide * wide, -1, keepdims=True) + 1e-6)
        for j, p in enumerate((s, s1, s2, s3)):
            cols = pl.ds(pl.multiple_of(p * PIECE, PIECE), PIECE)
            a = x_s[slot, :, cols].astype(F32) * scale * gain_ref[:, cols].astype(F32)
            a_s[pl.ds(pl.multiple_of(n * XR, XR), XR), j * PIECE : (j + 1) * PIECE] = a.astype(BF16)

    lax.fori_loop(0, steps, norm, None)

    def head_cols(h):
        return pl.ds(pl.multiple_of(h * HEAD, HEAD), HEAD)

    gathers[0].own().wait_recv()
    local_copy(0).wait()

    def begin(n, _):
        gathers[0].pass_x(n)
        for h in range(2):
            cols = head_cols(2 * n + h)

            for r in range(TOK // STRIP):
                rows = pl.ds(r * STRIP, STRIP)
                p_s[rows, cols] = _dot(a_s[rows, : 2 * PIECE], w_s[0, : 2 * PIECE, cols])

    lax.fori_loop(0, NCH, begin, None)

    def table(n, _):
        at = pl.ds(pl.multiple_of(n * FINE, FINE), FINE)
        fc, fs = far_ref[0, pl.ds(n, 1), :], far_ref[1, pl.ds(n, 1), :]
        cos_s[at, :] = fc * near_ref[0] - fs * near_ref[1]
        sin_s[at, :] = fs * near_ref[0] + fc * near_ref[1]

    lax.fori_loop(0, TOK // FINE, table, None)
    for n in range(NCH):
        gathers[0].pass_y(n)

    outs = (qt_ref, k_ref, vt_ref)
    here = pl.ds(pl.multiple_of(core * TOK, TOK), TOK)

    def stage(m):
        return k_s if m == 1 else t_s

    def out(m, n):
        return outs[m].at[n, here, :] if m == 1 else outs[m].at[n, :, here]

    def sent(m, n):
        slot = lax.rem(n, 2)
        return _remote(stage(m).at[slot], out(m, n), slot_sem.at[0, slot], to_sem.at[m, n], beside)

    def kept(m, n):
        slot = lax.rem(n, 2)
        return pltpu.make_async_copy(stage(m).at[2 + slot], out(m, n), slot_sem.at[1, slot])

    def ask(p):
        return _remote(qt_ref.at[:, :, _cols(_early(core, p))], ask_ref.at[p], as_sem.at[p], ar_sem.at[p], across)

    def make(m, h, slot):
        cols = head_cols(h)
        for r in range(TOK // STRIP):
            rows = pl.ds(r * STRIP, STRIP)
            if m == 0:
                t = p_s[rows, cols] + _dot(a_s[rows, 2 * PIECE :], w_s[m, 2 * PIECE :, cols])
            else:
                t = _dot(a_s[rows, :], w_s[m, :, cols])
            t = t.astype(BF16)
            if m < 2:
                t = t.astype(F32)
                lo, hi = t[:, : HEAD // 2], t[:, HEAD // 2 :]
                cos, sin = cos_s[rows, :], sin_s[rows, :]
                t = jnp.concatenate([lo * cos - hi * sin, hi * cos + lo * sin], axis=1).astype(BF16)
            if m == 1:
                k_s[slot, rows, :] = t
            else:
                t_s[slot, :, rows] = t.T

    for m in range(3):
        gathers[m].arrived()
        if m:
            gathers[m].own().wait_recv()
            local_copy(m).wait()

        def head(n, _):
            i = lax.rem(n, OWN)
            home = n >= OWN

            @pl.when((i >= 2) & jnp.logical_not(home))
            def _():
                sent(m, i - 2).wait_send()

            @pl.when((i >= 2) & home)
            def _():
                kept(m, i - 2).wait()

            if m < 2:
                pl.when(home)(lambda: gathers[m + 1].pass_y(i))
            make(m, lax.rem((1 - core) * OWN + n, HEADS), lax.rem(n, 2) + 2 * lax.div(n, OWN))

            @pl.when(home)
            def _():
                kept(m, i).start()

            @pl.when(jnp.logical_not(home))
            def _():
                sent(m, i).start()
                if m < 2:
                    gathers[m + 1].pass_x(i)

        lax.fori_loop(0, HEADS, head, None)
        for n in (OWN - 2, OWN - 1):
            sent(m, n).wait_send()
            kept(m, n).wait()
        if m == 0:

            @pl.when(jnp.logical_not(first_chip))
            def _():
                for p in range(EARLY):
                    ask(p).start()

    for g in gathers:
        g.left()
    for m in range(3):
        for n in range(OWN):
            sent(m, n).wait_recv()

    @pl.when(first_chip)
    def _():
        for p in range(EARLY):
            ask(p).wait_recv()

    @pl.when(jnp.logical_not(first_chip))
    def _():
        for p in range(EARLY):
            ask(p).wait_send()


def project(x, gain, far, near, wq, wk, wv):
    hbm, vmem = pl.BlockSpec(memory_space=pltpu.HBM), pl.BlockSpec(memory_space=pltpu.VMEM)
    dma = pltpu.SemaphoreType.DMA
    return pl.pallas_call(
        _project,
        in_specs=[hbm, vmem, vmem, vmem, hbm, hbm, hbm],
        out_specs=[hbm] * 4,
        out_shape=[
            jax.ShapeDtypeStruct((OWN, HEAD, CHIP), BF16),
            jax.ShapeDtypeStruct((OWN, CHIP, HEAD), BF16),
            jax.ShapeDtypeStruct((OWN, HEAD, CHIP), BF16),
            jax.ShapeDtypeStruct((EARLY, OWN, HEAD, STRIP), BF16),
        ],
        scratch_shapes=[
            pltpu.VMEM((TOK, D), BF16),
            pltpu.VMEM((2, 256, D), BF16),
            pltpu.VMEM((3, D, D), BF16),
            pltpu.VMEM((TOK, D), F32),
            pltpu.VMEM((4, HEAD, TOK), BF16),
            pltpu.VMEM((4, TOK, HEAD), BF16),
            pltpu.VMEM((TOK, HEAD // 2), F32),
            pltpu.VMEM((TOK, HEAD // 2), F32),
            dma((2,)), dma((3,)), dma((2, 2)), dma((3, OWN)), dma((EARLY,)), dma((EARLY,)),
            *_gather_sems(3),
        ],
        compiler_params=pltpu.CompilerParams(collective_id=0, has_side_effects=True, vmem_limit_bytes=VMEM),
        cost_estimate=pl.CostEstimate(flops=6 * TOK * D * D, transcendentals=0, bytes_accessed=64 * 2**20),
        name="project",
    )(x, gain, far, near, wq, wk, wv)


def _attend(qt_ref, k_ref, vt_ref, ask_ref, wo_ref, seen_ref, rest_ref,
            q_s, k_s, v_s, far_s, mix_s, top_s, part_s, lse_s, flse_s, seen_s, sa_s, sb_s,
            in_sem, q_sem, f_sem, qs_sem, qr_sem, ps_sem, pr_sem, ls_sem, lr_sem, slot_sem, to_sem, *g_sem):
    dp, s, core, s1, s2, _ = _places()
    beside, across, other = (dp, s1), (dp, s2), (1 - dp, s)
    first_chip = s < 2
    e = SCALE * LOG2E
    _greet((beside, across, other))
    wo = _Gather(wo_ref, lambda row, n: rest_ref.at[pl.ds(row - PIECE, n)], g_sem, 0)
    cols = _cols

    def early(p):
        return _early(core, p)

    def place(p):
        return jnp.where(p < NS // 2, (1 - core) * (NS // 2) + NS // 2 - 1 - p, core * (NS // 2) + NS - 1 - p)

    def ask(p):
        at = cols(early(p))
        return _remote(qt_ref.at[:, :, at], far_s.at[:, :, at], qs_sem.at[p], qr_sem.at[p], across)

    def asked(p):
        return pltpu.make_async_copy(ask_ref.at[p], far_s.at[:, :, cols(early(p))], f_sem.at[p])

    def answer(p):
        slot = lax.rem(p, 2)
        return (_remote(part_s.at[slot], far_s.at[:, :, cols(early(p))], ps_sem.at[slot], pr_sem.at[p], across),
                _remote(lse_s.at[slot], flse_s.at[p], ls_sem.at[slot], lr_sem.at[p], across))

    def q_in(p):
        slot = lax.rem(p, 2)
        return pltpu.make_async_copy(qt_ref.at[:, :, cols(place(p))], q_s.at[slot], q_sem.at[slot])

    def ours(t):
        return lax.div(t, NS // 2) == core

    def target(t):
        return seen_ref.at[pl.ds(core * OWN, OWN), cols(lax.rem(t, NS // 2))]

    def sent(t, slot):
        return _remote(seen_s.at[slot], target(t), slot_sem.at[slot], to_sem.at[lax.rem(t, NS // 2)], beside)

    def kept(t, slot):
        return pltpu.make_async_copy(seen_s.at[slot], target(t), slot_sem.at[slot])

    def hand(t, slot):
        @pl.when(ours(t))
        def _():
            kept(t, slot).start()

        @pl.when(jnp.logical_not(ours(t)))
        def _():
            sent(t, slot).start()

    def handed(t, slot):
        @pl.when(ours(t))
        def _():
            kept(t, slot).wait()

        @pl.when(jnp.logical_not(ours(t)))
        def _():
            sent(t, slot).wait_send()

    keys = pltpu.make_async_copy(k_ref, k_s, in_sem.at[0])
    values = pltpu.make_async_copy(vt_ref, v_s, in_sem.at[1])
    q_in(0).start()
    keys.start()
    values.start()

    @pl.when(jnp.logical_not(first_chip))
    def _():
        for p in range(EARLY, NS):
            ask(p).start()
        wo.start_x()

    @pl.when(first_chip)
    def _():
        wo.start_x()
        for p in range(EARLY):
            asked(p).start()

    wo.own().start()

    keys.wait()
    values.wait()
    ones = jnp.ones((8, STRIP), BF16)

    def clear(t):
        for i in range(OWN):
            top_s[i : i + 1, cols(t)] = jnp.full((1, STRIP), NEG, F32)
            mix_s[i, :, cols(t)] = jnp.zeros((HEAD + 8, STRIP), F32)

    def run(t, query, masked, count):
        def score(i, j, into):
            into[i] = _dot(k_s[i, cols(j), :], query(i))

        def fold(i, j, held, cut):
            sc = held[i]
            if cut:
                query_at, key_at = (lax.broadcasted_iota(jnp.int32, (STRIP, STRIP), n) for n in (1, 0))
                sc = jnp.where(query_at >= key_at, sc, HIDDEN)
            old = top_s[i : i + 1, cols(t)]
            top = jnp.maximum(old, sc.max(axis=0, keepdims=True))
            top_s[i : i + 1, cols(t)] = top
            weights = jnp.exp2((sc - top) * e).astype(BF16)
            keep = jnp.exp2((old - top) * e)
            val = jnp.concatenate([v_s[i, :, cols(j)], ones], axis=0)
            mix_s[i, :, cols(t)] = mix_s[i, :, cols(t)] * keep + _dot(val, weights)

        def step(j, held, after, into, cut=False):
            for i in range(OWN):
                if after is not None:
                    score(i, after, into)
                fold(i, j, held, cut)

        def pair(n, _):
            step(2 * n, sa_s, 2 * n + 1, sb_s)
            step(2 * n + 1, sb_s, 2 * n + 2, sa_s)

        def single():
            step(count - 1, sa_s, None, None)

        def double():
            step(count - 2, sa_s, count - 1, sb_s)
            step(count - 1, sb_s, None, None)

        clear(t)
        if masked:
            for i in range(OWN):
                score(i, t, sb_s)
            step(t, sb_s, 0, sa_s, True)
            lax.fori_loop(0, lax.div(jnp.maximum(count - 1, 0), 2), pair, None)
            pl.when(lax.rem(count, 2) == 1)(single)
            pl.when((lax.rem(count, 2) == 0) & (count > 0))(double)
        else:
            for i in range(OWN):
                score(i, 0, sa_s)
            lax.fori_loop(0, (count - 1) // 2, pair, None)
            double()

    def own(p):
        t, slot = place(p), lax.rem(p, 2)

        @pl.when(p + 1 < NS)
        def _():
            q_in(p + 1).start()

        q_in(p).wait()
        run(t, lambda i: q_s[slot, i], True, t)

    def cross(p):
        t = early(p)

        @pl.when(p < EARLY)
        def _():
            asked(p).wait()

        @pl.when(p >= EARLY)
        def _():
            ask(p).wait_recv()

        slot = lax.rem(p, 2)
        run(t, lambda i: far_s[i, :, cols(t)], False, NS)

        @pl.when(p >= 2)
        def _():
            for c in answer(p - 2):
                c.wait_send()

        for i in range(OWN):
            total = mix_s[i, HEAD : HEAD + 1, cols(t)]
            part_s[slot, i] = (mix_s[i, :HEAD, cols(t)] * (1 / total)).astype(BF16)
            lse_s[slot, i : i + 1, :] = top_s[i : i + 1, cols(t)] * SCALE + jnp.log(total)
        for c in answer(p):
            c.start()

    def finish(p):
        t, slot = place(p), lax.rem(p, 2)

        @pl.when(p >= 2)
        def _():
            handed(place(p - 2), slot)

        for i in range(OWN):
            total = mix_s[i, HEAD : HEAD + 1, cols(t)]
            seen_s[slot, i] = (mix_s[i, :HEAD, cols(t)] * (1 / total)).T.astype(BF16)
        hand(t, slot)

    def join(p):
        t, slot = early(p), lax.rem(p, 2)

        @pl.when(p >= 2)
        def _():
            handed(early(p - 2), slot)

        for i in range(OWN):
            total = mix_s[i, HEAD : HEAD + 1, cols(t)]
            mine = top_s[i : i + 1, cols(t)] * SCALE + jnp.log(total)
            theirs = flse_s[p, i : i + 1, :]
            top = jnp.maximum(mine, theirs)
            wm, wt = jnp.exp(mine - top), jnp.exp(theirs - top)
            both = 1 / (wm + wt)
            mixed = mix_s[i, :HEAD, cols(t)] * (wm * both / total) + far_s[i, :, cols(t)].astype(F32) * (wt * both)
            seen_s[slot, i] = mixed.T.astype(BF16)
        hand(t, slot)

    def step(p, _):
        @pl.when(first_chip)
        def _():
            cross(p)

        own(p)

        @pl.when(first_chip)
        def _():
            finish(p)

    lax.fori_loop(0, NS, step, None)
    for n in range(NCH):
        wo.pass_x(n)
    for n in range(NCH):
        wo.pass_y(n)

    @pl.when(first_chip)
    def _():
        for p in (NS - 2, NS - 1):
            for c in answer(p):
                c.wait_send()
            handed(place(p), p % 2)

    @pl.when(jnp.logical_not(first_chip))
    def _():
        for p in range(EARLY, NS):
            ask(p).wait_send()

        def merge(p, _):
            for c in answer(p):
                c.wait_recv()
            join(p)

        lax.fori_loop(0, NS, merge, None)
        for p in (NS - 2, NS - 1):
            handed(early(p), p % 2)

    for n in range(NS // 2):
        sent(n, 0).wait_recv()
    wo.own().wait_recv()
    wo.arrived()
    wo.left()


def attend(qt, k, vt, asked, wo):
    hbm = pl.BlockSpec(memory_space=pltpu.HBM)
    dma = pltpu.SemaphoreType.DMA
    return pl.pallas_call(
        _attend,
        in_specs=[hbm] * 5,
        out_specs=[hbm] * 2,
        out_shape=[jax.ShapeDtypeStruct((HEADS, TOK, HEAD), BF16), jax.ShapeDtypeStruct((3 * PIECE, D), BF16)],
        scratch_shapes=[
            pltpu.VMEM((2, OWN, HEAD, STRIP), BF16),
            pltpu.VMEM((OWN, CHIP, HEAD), BF16),
            pltpu.VMEM((OWN, HEAD, CHIP), BF16),
            pltpu.VMEM((OWN, HEAD, CHIP), BF16),
            pltpu.VMEM((OWN, HEAD + 8, CHIP), F32),
            pltpu.VMEM((OWN, CHIP), F32),
            pltpu.VMEM((2, OWN, HEAD, STRIP), BF16),
            pltpu.VMEM((2, OWN, STRIP), F32),
            pltpu.VMEM((NS, OWN, STRIP), F32),
            pltpu.VMEM((2, OWN, STRIP, HEAD), BF16),
            pltpu.VMEM((OWN, STRIP, STRIP), F32),
            pltpu.VMEM((OWN, STRIP, STRIP), F32),
            dma((2,)), dma((2,)), dma((EARLY,)), dma((NS,)), dma((NS,)), dma((2,)), dma((NS,)), dma((2,)), dma((NS,)), dma((2,)),
            dma((NS // 2,)),
            *_gather_sems(1),
        ],
        compiler_params=pltpu.CompilerParams(collective_id=1, has_side_effects=True, vmem_limit_bytes=VMEM),
        cost_estimate=pl.CostEstimate(flops=6 * OWN * CHIP * CHIP * HEAD, transcendentals=OWN * CHIP * CHIP, bytes_accessed=64 * 2**20),
        name="attend",
    )(qt, k, vt, asked, wo)


def _output(seen_ref, x_ref, wo_ref, rest_ref, y_ref):
    _, s, _, s1, s2, s3 = _places()
    lhs = jnp.concatenate([seen_ref[p * 2 + i] for p in (s, s1, s2, s3) for i in range(2)], axis=1)
    for n in range(D // 512):
        at = slice(n * 512, (n + 1) * 512)
        w = jnp.concatenate([wo_ref[:, at], rest_ref[:, at]], axis=0)
        y_ref[:, at] = (x_ref[:, at].astype(F32) + _dot(lhs, w)).astype(BF16)


def output(seen, x, wo, rest):
    rows = 512
    return pl.pallas_call(
        _output,
        grid=(TOK // rows,),
        in_specs=[
            pl.BlockSpec((HEADS, rows, HEAD), lambda i: (0, i, 0)),
            pl.BlockSpec((rows, D), lambda i: (i, 0)),
            pl.BlockSpec((PIECE, D), lambda i: (0, 0)),
            pl.BlockSpec((3 * PIECE, D), lambda i: (0, 0)),
        ],
        out_specs=pl.BlockSpec((rows, D), lambda i: (i, 0)),
        out_shape=jax.ShapeDtypeStruct((TOK, D), BF16),
        compiler_params=pltpu.CompilerParams(dimension_semantics=("arbitrary",), vmem_limit_bytes=56 * 2**20),
        cost_estimate=pl.CostEstimate(flops=2 * TOK * D * D, transcendentals=0, bytes_accessed=32 * 2**20),
        name="output",
    )(seen, x, wo, rest)


def solution(mesh):
    def step(x, gain, wq, wk, wv, wo):
        s = lax.axis_index("sp")
        rate = THETA ** (-jnp.arange(HEAD // 2, dtype=F32) / (HEAD // 2))

        def table(place):
            angle = place.astype(F32)[:, None] * rate
            return jnp.stack([jnp.cos(angle), jnp.sin(angle)])

        far, near = table(s * TOK + FINE * jnp.arange(TOK // FINE)), table(jnp.arange(FINE))
        qt, k, vt, asked = project(x, gain[None], far, near, wq, wk, wv)
        seen, rest = attend(qt, k, vt, asked, wo)
        return output(seen, x, wo, rest)

    tokens, whole = P(("dp", "sp"), None), P("sp", None)
    return jax.shard_map(
        step,
        mesh=mesh,
        in_specs=(tokens, P(None), whole, whole, whole, whole),
        out_specs=tokens,
        check_vma=False,
    )
```

```python
import functools

import jax
import jax.numpy as jnp
from jax import lax
from jax.experimental import pallas as pl
from jax.experimental.pallas import tpu as pltpu
from jax.sharding import PartitionSpec as P

NEG = -1e30
HIDDEN = 2 * NEG
LOG2E = 1.4426950408889634
HEAD = 256
HEADS = 8
OWN = 4
D = 2048
TOK = 2048
CHIP = 2 * TOK
PIECE = D // 4
HALF = PIECE // 2
NCH = 4
CH = HALF // NCH
STRIP = 512
NS = CHIP // STRIP
THETA = 10000
EARLY = 1
FINE = 64
SCALE = HEAD**-0.5
MESH = pl.DeviceIdType.MESH
VMEM = 63 * 2**20
F32, BF16 = jnp.float32, jnp.bfloat16


def _places():
    dp, s = lax.axis_index("dp"), lax.axis_index("sp")
    core = lax.rem(s, 2)
    s1 = s + 1 - 2 * core
    s2, s3 = lax.rem(s + 2, 4), lax.rem(s1 + 2, 4)
    return dp, s, core, s1, s2, s3


def _greet(devices):
    barrier = pltpu.get_barrier_semaphore()
    for d in devices:
        pl.semaphore_signal(barrier, inc=1, device_id=d, device_id_type=MESH)
    pl.semaphore_wait(barrier, len(devices))


def _remote(src, dst, send, recv, device):
    return pltpu.make_async_remote_copy(src_ref=src, dst_ref=dst, send_sem=send, recv_sem=recv, device_id=device, device_id_type=MESH)


def _dot(a, b):
    return jnp.dot(a, b, preferred_element_type=F32)


class _Gather:
    def __init__(self, w_ref, held, sems, m):
        dp, s, core, s1, s2, s3 = _places()
        own_send, own_recv, x_send, x_recv, y_send, y_recv, d_send, d_recv, e_send, e_recv = sems
        beside, across, other = (dp, s1), (dp, s2), (1 - dp, s)
        mine, theirs = dp * HALF, (1 - dp) * HALF

        def own(n=None):
            return _remote(w_ref, held(PIECE, PIECE), own_send.at[m], own_recv.at[m], beside)

        def x(n):
            return _remote(w_ref.at[pl.ds(mine + n * CH, CH)], held(2 * PIECE + mine + n * CH, CH), x_send.at[m, n], x_recv.at[m, n], across)

        def y(n):
            at = 2 * PIECE + mine + n * CH
            return _remote(held(at, CH), held(at, CH), y_send.at[m, n], y_recv.at[m, n], other)

        def d(n):
            at = 2 * PIECE + mine + n * CH
            return _remote(held(at, CH), held(PIECE + at, CH), d_send.at[m, n], d_recv.at[m, n], beside)

        def e(n):
            at = 2 * PIECE + theirs + n * CH
            return _remote(held(at, CH), held(PIECE + at, CH), e_send.at[m, n], e_recv.at[m, n], beside)

        self.own, self.x, self.y, self.d, self.e = own, x, y, d, e

    def start_x(self):
        for n in range(NCH):
            self.x(n).start()

    def pass_x(self, n):
        self.x(n).wait_recv()
        self.y(n).start()
        self.d(n).start()

    def pass_y(self, n):
        self.y(n).wait_recv()
        self.e(n).start()

    def arrived(self):
        for n in range(NCH):
            self.d(n).wait_recv()
            self.e(n).wait_recv()

    def left(self):
        self.own().wait_send()
        for n in range(NCH):
            self.x(n).wait_send()
        self.passed()

    def passed(self):
        for n in range(NCH):
            for c in (self.y, self.d, self.e):
                c(n).wait_send()


def _gather_sems(count):
    dma = pltpu.SemaphoreType.DMA
    return [dma((count,)), dma((count,))] + [dma((count, NCH)) for _ in range(8)]


def _early(core, p):
    return lax.rem(core * (NS // 2) + p, NS)


def _cols(t):
    return pl.ds(pl.multiple_of(t * STRIP, STRIP), STRIP)


def _project(x_ref, gain_ref, far_ref, near_ref, wq_ref, wk_ref, wv_ref, wo_ref, qt_ref, k_ref, vt_ref, ask_ref, rest_ref,
             a_s, x_s, w_s, p_s, t_s, k_s, cos_s, sin_s, x_sem, l_sem, slot_sem, to_sem, as_sem, ar_sem, *g_sem):
    dp, s, core, s1, s2, s3 = _places()
    beside, across, other = (dp, s1), (dp, s2), (1 - dp, s)
    first_chip = s < 2
    w_refs = (wq_ref, wk_ref, wv_ref)
    _greet((beside, across, other))
    gathers = [_Gather(w_refs[m], lambda row, n, m=m: w_s.at[m, pl.ds(row, n)], g_sem, m) for m in range(3)]
    wo = _Gather(wo_ref, lambda row, n: rest_ref.at[pl.ds(row - PIECE, n)], g_sem, 3)

    def local_copy(m):
        return pltpu.make_async_copy(w_refs[m], w_s.at[m, pl.ds(0, PIECE)], l_sem.at[m])

    XR = x_s.shape[1]
    steps = TOK // XR

    def x_in(n):
        return pltpu.make_async_copy(x_ref.at[pl.ds(n * XR, XR)], x_s.at[lax.rem(n, 2)], x_sem.at[lax.rem(n, 2)])

    x_in(0).start()
    for m in range(3):
        gathers[m].start_x()
    pl.when(first_chip)(wo.start_x)
    for m in range(3):
        gathers[m].own().start()
        local_copy(m).start()

    def norm(n, _):
        @pl.when(n + 1 < steps)
        def _():
            x_in(n + 1).start()

        x_in(n).wait()
        slot = lax.rem(n, 2)
        wide = x_s[slot].astype(F32)
        scale = lax.rsqrt(jnp.mean(wide * wide, -1, keepdims=True) + 1e-6)
        for j, p in enumerate((s, s1, s2, s3)):
            cols = pl.ds(pl.multiple_of(p * PIECE, PIECE), PIECE)
            a = x_s[slot, :, cols].astype(F32) * scale * gain_ref[:, cols].astype(F32)
            a_s[pl.ds(pl.multiple_of(n * XR, XR), XR), j * PIECE : (j + 1) * PIECE] = a.astype(BF16)

    lax.fori_loop(0, steps, norm, None)

    def head_cols(h):
        return pl.ds(pl.multiple_of(h * HEAD, HEAD), HEAD)

    gathers[0].own().wait_recv()
    local_copy(0).wait()

    def begin(n, _):
        gathers[0].pass_x(n)
        for h in range(HEADS // NCH):
            cols = head_cols(HEADS // NCH * n + h)

            for r in range(TOK // STRIP):
                rows = pl.ds(r * STRIP, STRIP)
                p_s[rows, cols] = _dot(a_s[rows, : 2 * PIECE], w_s[0, : 2 * PIECE, cols])

    lax.fori_loop(0, NCH, begin, None)

    def table(n, _):
        at = pl.ds(pl.multiple_of(n * FINE, FINE), FINE)
        fc, fs = far_ref[0, pl.ds(n, 1), :], far_ref[1, pl.ds(n, 1), :]
        cos_s[at, :] = fc * near_ref[0] - fs * near_ref[1]
        sin_s[at, :] = fs * near_ref[0] + fc * near_ref[1]

    lax.fori_loop(0, TOK // FINE, table, None)
    for n in range(NCH):
        gathers[0].pass_y(n)

    outs = (qt_ref, k_ref, vt_ref)
    here = pl.ds(pl.multiple_of(core * TOK, TOK), TOK)

    def stage(m):
        return k_s if m == 1 else t_s

    def out(m, n):
        return outs[m].at[n, here, :] if m == 1 else outs[m].at[n, :, here]

    def sent(m, n):
        slot = lax.rem(n, 2)
        return _remote(stage(m).at[slot], out(m, n), slot_sem.at[0, slot], to_sem.at[m, n], beside)

    def kept(m, n):
        slot = lax.rem(n, 2)
        return pltpu.make_async_copy(stage(m).at[2 + slot], out(m, n), slot_sem.at[1, slot])

    def ask(p):
        return _remote(qt_ref.at[:, :, _cols(_early(core, p))], ask_ref.at[p], as_sem.at[p], ar_sem.at[p], across)

    def make(m, h, slot):
        cols = head_cols(h)
        for r in range(TOK // STRIP):
            rows = pl.ds(r * STRIP, STRIP)
            if m == 0:
                t = p_s[rows, cols] + _dot(a_s[rows, 2 * PIECE :], w_s[m, 2 * PIECE :, cols])
            else:
                t = _dot(a_s[rows, :], w_s[m, :, cols])
            t = t.astype(BF16)
            if m < 2:
                t = t.astype(F32)
                lo, hi = t[:, : HEAD // 2], t[:, HEAD // 2 :]
                cos, sin = cos_s[rows, :], sin_s[rows, :]
                t = jnp.concatenate([lo * cos - hi * sin, hi * cos + lo * sin], axis=1).astype(BF16)
            if m == 1:
                k_s[slot, rows, :] = t
            else:
                t_s[slot, :, rows] = t.T

    for m in range(3):
        gathers[m].arrived()
        if m:
            gathers[m].own().wait_recv()
            local_copy(m).wait()

        def head(n, _):
            i = lax.rem(n, OWN)
            home = n >= OWN

            @pl.when((i >= 2) & jnp.logical_not(home))
            def _():
                sent(m, i - 2).wait_send()

            @pl.when((i >= 2) & home)
            def _():
                kept(m, i - 2).wait()

            if m < 2:

                @pl.when(home)
                def _():
                    for c in range(NCH // OWN):
                        gathers[m + 1].pass_y(i * (NCH // OWN) + c)

            make(m, lax.rem((1 - core) * OWN + n, HEADS), lax.rem(n, 2) + 2 * lax.div(n, OWN))

            @pl.when(home)
            def _():
                kept(m, i).start()

            @pl.when(jnp.logical_not(home))
            def _():
                sent(m, i).start()
                if m < 2:
                    for c in range(NCH // OWN):
                        gathers[m + 1].pass_x(i * (NCH // OWN) + c)

        lax.fori_loop(0, HEADS, head, None)
        for n in (OWN - 2, OWN - 1):
            sent(m, n).wait_send()
            kept(m, n).wait()
        if m == 0:

            @pl.when(jnp.logical_not(first_chip))
            def _():
                for p in range(EARLY):
                    ask(p).start()

    for g in gathers:
        g.left()
    for m in range(3):
        for n in range(OWN):
            sent(m, n).wait_recv()

    @pl.when(first_chip)
    def _():
        for n in range(NCH):
            wo.x(n).wait_send()
        for p in range(EARLY):
            ask(p).wait_recv()

    @pl.when(jnp.logical_not(first_chip))
    def _():
        for n in range(NCH):
            wo.x(n).wait_recv()
        for p in range(EARLY):
            ask(p).wait_send()


def project(x, gain, far, near, wq, wk, wv, wo):
    hbm, vmem = pl.BlockSpec(memory_space=pltpu.HBM), pl.BlockSpec(memory_space=pltpu.VMEM)
    dma = pltpu.SemaphoreType.DMA
    return pl.pallas_call(
        _project,
        in_specs=[hbm, vmem, vmem, vmem, hbm, hbm, hbm, hbm],
        out_specs=[hbm] * 5,
        out_shape=[
            jax.ShapeDtypeStruct((OWN, HEAD, CHIP), BF16),
            jax.ShapeDtypeStruct((OWN, CHIP, HEAD), BF16),
            jax.ShapeDtypeStruct((OWN, HEAD, CHIP), BF16),
            jax.ShapeDtypeStruct((EARLY, OWN, HEAD, STRIP), BF16),
            jax.ShapeDtypeStruct((3 * PIECE, D), BF16),
        ],
        scratch_shapes=[
            pltpu.VMEM((TOK, D), BF16),
            pltpu.VMEM((2, 256, D), BF16),
            pltpu.VMEM((3, D, D), BF16),
            pltpu.VMEM((TOK, D), F32),
            pltpu.VMEM((4, HEAD, TOK), BF16),
            pltpu.VMEM((4, TOK, HEAD), BF16),
            pltpu.VMEM((TOK, HEAD // 2), F32),
            pltpu.VMEM((TOK, HEAD // 2), F32),
            dma((2,)), dma((3,)), dma((2, 2)), dma((3, OWN)), dma((EARLY,)), dma((EARLY,)),
            *_gather_sems(4),
        ],
        compiler_params=pltpu.CompilerParams(collective_id=0, has_side_effects=True, vmem_limit_bytes=VMEM),
        cost_estimate=pl.CostEstimate(flops=6 * TOK * D * D, transcendentals=0, bytes_accessed=64 * 2**20),
        name="project",
    )(x, gain, far, near, wq, wk, wv, wo)


def _attend(qt_ref, k_ref, vt_ref, ask_ref, wo_ref, _, seen_ref, rest_ref,
            q_s, k_s, v_s, far_s, mix_s, top_s, part_s, lse_s, flse_s, seen_s, sa_s, sb_s,
            in_sem, q_sem, f_sem, qs_sem, qr_sem, ps_sem, pr_sem, ls_sem, lr_sem, slot_sem, to_sem, *g_sem):
    dp, s, core, s1, s2, _ = _places()
    beside, across, other = (dp, s1), (dp, s2), (1 - dp, s)
    first_chip = s < 2
    e = SCALE * LOG2E
    _greet((beside, across, other))
    wo = _Gather(wo_ref, lambda row, n: rest_ref.at[pl.ds(row - PIECE, n)], g_sem, 0)
    cols = _cols

    def early(p):
        return _early(core, p)

    def place(p):
        return jnp.where(p < NS // 2, (1 - core) * (NS // 2) + NS // 2 - 1 - p, core * (NS // 2) + NS - 1 - p)

    def ask(p):
        at = cols(early(p))
        return _remote(qt_ref.at[:, :, at], far_s.at[:, :, at], qs_sem.at[p], qr_sem.at[p], across)

    def asked(p):
        return pltpu.make_async_copy(ask_ref.at[p], far_s.at[:, :, cols(early(p))], f_sem.at[p])

    def answer(p):
        return [c for half in range(2) for c in answered(p, half)]

    def answered(p, half):
        slot, heads = lax.rem(p, 2), pl.ds(2 * half, 2)
        return (_remote(part_s.at[slot, heads], far_s.at[heads, :, cols(early(p))], ps_sem.at[slot, half], pr_sem.at[p, half], across),
                _remote(lse_s.at[slot, half], flse_s.at[p, half], ls_sem.at[slot, half], lr_sem.at[p, half], across))

    def q_in(p):
        slot = lax.rem(p, 2)
        return pltpu.make_async_copy(qt_ref.at[:, :, cols(place(p))], q_s.at[slot], q_sem.at[slot])

    def ours(t):
        return lax.div(t, NS // 2) == core

    def target(t):
        return seen_ref.at[pl.ds(core * OWN, OWN), cols(lax.rem(t, NS // 2))]

    def sent(t, slot):
        return _remote(seen_s.at[slot], target(t), slot_sem.at[slot], to_sem.at[lax.rem(t, NS // 2)], beside)

    def kept(t, slot):
        return pltpu.make_async_copy(seen_s.at[slot], target(t), slot_sem.at[slot])

    def hand(t, slot):
        @pl.when(ours(t))
        def _():
            kept(t, slot).start()

        @pl.when(jnp.logical_not(ours(t)))
        def _():
            sent(t, slot).start()

    def handed(t, slot):
        @pl.when(ours(t))
        def _():
            kept(t, slot).wait()

        @pl.when(jnp.logical_not(ours(t)))
        def _():
            sent(t, slot).wait_send()

    keys = pltpu.make_async_copy(k_ref, k_s, in_sem.at[0])
    values = pltpu.make_async_copy(vt_ref, v_s, in_sem.at[1])
    q_in(0).start()
    keys.start()
    values.start()

    @pl.when(jnp.logical_not(first_chip))
    def _():
        for p in range(EARLY, NS):
            ask(p).start()
        wo.start_x()
        for n in range(NCH):
            wo.y(n).start()
            wo.d(n).start()

    @pl.when(first_chip)
    def _():
        for p in range(EARLY):
            asked(p).start()

    wo.own().start()

    keys.wait()
    values.wait()
    ones = jnp.ones((8, STRIP), BF16)

    def clear(t, heads):
        for i in heads:
            top_s[i : i + 1, cols(t)] = jnp.full((1, STRIP), NEG, F32)
            mix_s[i, :, cols(t)] = jnp.zeros((HEAD + 8, STRIP), F32)

    def run(t, query, masked, count, heads=range(OWN)):
        def score(i, j, into):
            into[i] = _dot(k_s[i, cols(j), :], query(i))

        def fold(i, j, held, cut):
            sc = held[i]
            if cut:
                query_at, key_at = (lax.broadcasted_iota(jnp.int32, (STRIP, STRIP), n) for n in (1, 0))
                sc = jnp.where(query_at >= key_at, sc, HIDDEN)
            old = top_s[i : i + 1, cols(t)]
            top = jnp.maximum(old, sc.max(axis=0, keepdims=True))
            top_s[i : i + 1, cols(t)] = top
            weights = jnp.exp2((sc - top) * e).astype(BF16)
            keep = jnp.exp2((old - top) * e)
            val = jnp.concatenate([v_s[i, :, cols(j)], ones], axis=0)
            mix_s[i, :, cols(t)] = mix_s[i, :, cols(t)] * keep + _dot(val, weights)

        def step(j, held, after, into, cut=False):
            for i in heads:
                if after is not None:
                    score(i, after, into)
                fold(i, j, held, cut)

        def pair(n, _):
            step(2 * n, sa_s, 2 * n + 1, sb_s)
            step(2 * n + 1, sb_s, 2 * n + 2, sa_s)

        def single():
            step(count - 1, sa_s, None, None)

        def double():
            step(count - 2, sa_s, count - 1, sb_s)
            step(count - 1, sb_s, None, None)

        clear(t, heads)
        if masked:
            for i in heads:
                score(i, t, sb_s)
            step(t, sb_s, 0, sa_s, True)
            lax.fori_loop(0, lax.div(jnp.maximum(count - 1, 0), 2), pair, None)
            pl.when(lax.rem(count, 2) == 1)(single)
            pl.when((lax.rem(count, 2) == 0) & (count > 0))(double)
        else:
            for i in heads:
                score(i, 0, sa_s)
            lax.fori_loop(0, (count - 1) // 2, pair, None)
            double()

    def own(p):
        t, slot = place(p), lax.rem(p, 2)

        @pl.when(p + 1 < NS)
        def _():
            q_in(p + 1).start()

        q_in(p).wait()
        run(t, lambda i: q_s[slot, i], True, t)

    def cross(p):
        t = early(p)

        @pl.when(p < EARLY)
        def _():
            asked(p).wait()

        @pl.when(p >= EARLY)
        def _():
            ask(p).wait_recv()

        slot = lax.rem(p, 2)
        for half in range(2):
            heads = (2 * half, 2 * half + 1)
            run(t, lambda i: far_s[i, :, cols(t)], False, NS, heads)

            @pl.when(p >= 2)
            def _():
                for c in answered(p - 2, half):
                    c.wait_send()

            for i in heads:
                total = mix_s[i, HEAD : HEAD + 1, cols(t)]
                part_s[slot, i] = (mix_s[i, :HEAD, cols(t)] * (1 / total)).astype(BF16)
                lse_s[slot, half, i % 2 : i % 2 + 1, :] = top_s[i : i + 1, cols(t)] * SCALE + jnp.log(total)
            for c in answered(p, half):
                c.start()

    def finish(p):
        t, slot = place(p), lax.rem(p, 2)

        @pl.when(p >= 2)
        def _():
            handed(place(p - 2), slot)

        for i in range(OWN):
            total = mix_s[i, HEAD : HEAD + 1, cols(t)]
            seen_s[slot, i] = (mix_s[i, :HEAD, cols(t)] * (1 / total)).T.astype(BF16)
        hand(t, slot)

    def join(p):
        t, slot = early(p), lax.rem(p, 2)

        @pl.when(p >= 2)
        def _():
            handed(early(p - 2), slot)

        for i in range(OWN):
            total = mix_s[i, HEAD : HEAD + 1, cols(t)]
            mine = top_s[i : i + 1, cols(t)] * SCALE + jnp.log(total)
            theirs = flse_s[p, i // 2, i % 2 : i % 2 + 1, :]
            top = jnp.maximum(mine, theirs)
            wm, wt = jnp.exp(mine - top), jnp.exp(theirs - top)
            both = 1 / (wm + wt)
            mixed = mix_s[i, :HEAD, cols(t)] * (wm * both / total) + far_s[i, :, cols(t)].astype(F32) * (wt * both)
            seen_s[slot, i] = mixed.T.astype(BF16)
        hand(t, slot)

    def step(p, _):
        @pl.when(first_chip)
        def _():
            cross(p)

        own(p)

        @pl.when(first_chip)
        def _():
            finish(p)

    lax.fori_loop(0, NS, step, None)

    @pl.when(first_chip)
    def _():
        for n in range(NCH):
            wo.pass_x(n)

    for n in range(NCH):
        wo.pass_y(n)

    @pl.when(first_chip)
    def _():
        for p in (NS - 2, NS - 1):
            for c in answer(p):
                c.wait_send()
            handed(place(p), p % 2)

    @pl.when(jnp.logical_not(first_chip))
    def _():
        for p in range(EARLY, NS):
            ask(p).wait_send()
        for n in range(NCH):
            wo.x(n).wait_send()

        def merge(p, _):
            for c in answer(p):
                c.wait_recv()
            join(p)

        lax.fori_loop(0, NS, merge, None)
        for p in (NS - 2, NS - 1):
            handed(early(p), p % 2)

    for n in range(NS // 2):
        sent(n, 0).wait_recv()
    wo.own().wait_recv()
    wo.own().wait_send()
    wo.arrived()
    wo.passed()


def attend(qt, k, vt, asked, wo, rest):
    hbm = pl.BlockSpec(memory_space=pltpu.HBM)
    dma = pltpu.SemaphoreType.DMA
    return pl.pallas_call(
        _attend,
        in_specs=[hbm] * 6,
        out_specs=[hbm] * 2,
        input_output_aliases={5: 1},
        out_shape=[jax.ShapeDtypeStruct((HEADS, TOK, HEAD), BF16), jax.ShapeDtypeStruct((3 * PIECE, D), BF16)],
        scratch_shapes=[
            pltpu.VMEM((2, OWN, HEAD, STRIP), BF16),
            pltpu.VMEM((OWN, CHIP, HEAD), BF16),
            pltpu.VMEM((OWN, HEAD, CHIP), BF16),
            pltpu.VMEM((OWN, HEAD, CHIP), BF16),
            pltpu.VMEM((OWN, HEAD + 8, CHIP), F32),
            pltpu.VMEM((OWN, CHIP), F32),
            pltpu.VMEM((2, OWN, HEAD, STRIP), BF16),
            pltpu.VMEM((2, 2, OWN // 2, STRIP), F32),
            pltpu.VMEM((NS, 2, OWN // 2, STRIP), F32),
            pltpu.VMEM((2, OWN, STRIP, HEAD), BF16),
            pltpu.VMEM((OWN, STRIP, STRIP), F32),
            pltpu.VMEM((OWN, STRIP, STRIP), F32),
            dma((2,)), dma((2,)), dma((EARLY,)), dma((NS,)), dma((NS,)), dma((2, 2)), dma((NS, 2)), dma((2, 2)), dma((NS, 2)), dma((2,)),
            dma((NS // 2,)),
            *_gather_sems(1),
        ],
        compiler_params=pltpu.CompilerParams(collective_id=1, has_side_effects=True, vmem_limit_bytes=VMEM),
        cost_estimate=pl.CostEstimate(flops=6 * OWN * CHIP * CHIP * HEAD, transcendentals=OWN * CHIP * CHIP, bytes_accessed=64 * 2**20),
        name="attend",
    )(qt, k, vt, asked, wo, rest)


def _output(seen_ref, x_ref, wo_ref, rest_ref, y_ref):
    _, s, _, s1, s2, s3 = _places()
    lhs = jnp.concatenate([seen_ref[p * 2 + i] for p in (s, s1, s2, s3) for i in range(2)], axis=1)
    for n in range(D // 512):
        at = slice(n * 512, (n + 1) * 512)
        w = jnp.concatenate([wo_ref[:, at], rest_ref[:, at]], axis=0)
        y_ref[:, at] = (x_ref[:, at].astype(F32) + _dot(lhs, w)).astype(BF16)


def output(seen, x, wo, rest):
    rows = 512
    return pl.pallas_call(
        _output,
        grid=(TOK // rows,),
        in_specs=[
            pl.BlockSpec((HEADS, rows, HEAD), lambda i: (0, i, 0)),
            pl.BlockSpec((rows, D), lambda i: (i, 0)),
            pl.BlockSpec((PIECE, D), lambda i: (0, 0)),
            pl.BlockSpec((3 * PIECE, D), lambda i: (0, 0)),
        ],
        out_specs=pl.BlockSpec((rows, D), lambda i: (i, 0)),
        out_shape=jax.ShapeDtypeStruct((TOK, D), BF16),
        compiler_params=pltpu.CompilerParams(dimension_semantics=("arbitrary",), vmem_limit_bytes=56 * 2**20),
        cost_estimate=pl.CostEstimate(flops=2 * TOK * D * D, transcendentals=0, bytes_accessed=32 * 2**20),
        name="output",
    )(seen, x, wo, rest)


def solution(mesh):
    def step(x, gain, wq, wk, wv, wo):
        s = lax.axis_index("sp")
        rate = THETA ** (-jnp.arange(HEAD // 2, dtype=F32) / (HEAD // 2))

        def table(place):
            angle = place.astype(F32)[:, None] * rate
            return jnp.stack([jnp.cos(angle), jnp.sin(angle)])

        far, near = table(s * TOK + FINE * jnp.arange(TOK // FINE)), table(jnp.arange(FINE))
        qt, k, vt, asked, rest = project(x, gain[None], far, near, wq, wk, wv, wo)
        seen, rest = attend(qt, k, vt, asked, wo, rest)
        return output(seen, x, wo, rest)

    tokens, whole = P(("dp", "sp"), None), P("sp", None)
    return jax.shard_map(
        step,
        mesh=mesh,
        in_specs=(tokens, P(None), whole, whole, whole, whole),
        out_specs=tokens,
        check_vma=False,
    )
```

```python
import functools

import jax
import jax.numpy as jnp
from jax import lax
from jax.experimental import pallas as pl
from jax.experimental.pallas import tpu as pltpu
from jax.sharding import PartitionSpec as P

NEG = -1e30
HIDDEN = 2 * NEG
LOG2E = 1.4426950408889634
HEAD = 256
HEADS = 8
OWN = 4
D = 2048
TOK = 2048
CHIP = 2 * TOK
PIECE = D // 4
HALF = PIECE // 2
NCH = 4
CH = HALF // NCH
STRIP = 512
NS = CHIP // STRIP
THETA = 10000
EARLY = 1
FINE = 64
SCALE = HEAD**-0.5
MESH = pl.DeviceIdType.MESH
VMEM = 63 * 2**20
F32, BF16 = jnp.float32, jnp.bfloat16


def _places():
    dp, s = lax.axis_index("dp"), lax.axis_index("sp")
    core = lax.rem(s, 2)
    s1 = s + 1 - 2 * core
    s2, s3 = lax.rem(s + 2, 4), lax.rem(s1 + 2, 4)
    return dp, s, core, s1, s2, s3


def _greet(devices):
    barrier = pltpu.get_barrier_semaphore()
    for d in devices:
        pl.semaphore_signal(barrier, inc=1, device_id=d, device_id_type=MESH)
    pl.semaphore_wait(barrier, len(devices))


def _remote(src, dst, send, recv, device):
    return pltpu.make_async_remote_copy(src_ref=src, dst_ref=dst, send_sem=send, recv_sem=recv, device_id=device, device_id_type=MESH)


def _dot(a, b):
    return jnp.dot(a, b, preferred_element_type=F32)


class _Gather:
    def __init__(self, w_ref, held, sems, m):
        dp, s, core, s1, s2, s3 = _places()
        own_send, own_recv, x_send, x_recv, y_send, y_recv, d_send, d_recv, e_send, e_recv = sems
        beside, across, other = (dp, s1), (dp, s2), (1 - dp, s)
        mine, theirs = dp * HALF, (1 - dp) * HALF

        def own(n=None):
            return _remote(w_ref, held(PIECE, PIECE), own_send.at[m], own_recv.at[m], beside)

        def x(n):
            return _remote(w_ref.at[pl.ds(mine + n * CH, CH)], held(2 * PIECE + mine + n * CH, CH), x_send.at[m, n], x_recv.at[m, n], across)

        def y(n):
            at = 2 * PIECE + mine + n * CH
            return _remote(held(at, CH), held(at, CH), y_send.at[m, n], y_recv.at[m, n], other)

        def d(n):
            at = 2 * PIECE + mine + n * CH
            return _remote(held(at, CH), held(PIECE + at, CH), d_send.at[m, n], d_recv.at[m, n], beside)

        def e(n):
            at = 2 * PIECE + theirs + n * CH
            return _remote(held(at, CH), held(PIECE + at, CH), e_send.at[m, n], e_recv.at[m, n], beside)

        self.own, self.x, self.y, self.d, self.e = own, x, y, d, e

    def start_x(self):
        for n in range(NCH):
            self.x(n).start()

    def pass_x(self, n):
        self.x(n).wait_recv()
        self.y(n).start()
        self.d(n).start()

    def pass_y(self, n):
        self.y(n).wait_recv()
        self.e(n).start()

    def arrived(self):
        for n in range(NCH):
            self.d(n).wait_recv()
            self.e(n).wait_recv()

    def left(self):
        self.own().wait_send()
        for n in range(NCH):
            self.x(n).wait_send()
        self.passed()

    def passed(self):
        for n in range(NCH):
            for c in (self.y, self.d, self.e):
                c(n).wait_send()


def _gather_sems(count):
    dma = pltpu.SemaphoreType.DMA
    return [dma((count,)), dma((count,))] + [dma((count, NCH)) for _ in range(8)]


def _early(core, p):
    return lax.rem(core * (NS // 2) + p, NS)


def _cols(t):
    return pl.ds(pl.multiple_of(t * STRIP, STRIP), STRIP)


def _project(x_ref, gain_ref, far_ref, near_ref, wq_ref, wk_ref, wv_ref, wo_ref, qt_ref, k_ref, vt_ref, ask_ref, rest_ref,
             a_s, x_s, w_s, p_s, t_s, k_s, cos_s, sin_s, x_sem, l_sem, slot_sem, to_sem, as_sem, ar_sem, *g_sem):
    dp, s, core, s1, s2, s3 = _places()
    beside, across, other = (dp, s1), (dp, s2), (1 - dp, s)
    first_chip = s < 2
    w_refs = (wq_ref, wk_ref, wv_ref)
    _greet((beside, across, other))
    gathers = [_Gather(w_refs[m], lambda row, n, m=m: w_s.at[m, pl.ds(row, n)], g_sem, m) for m in range(3)]
    wo = _Gather(wo_ref, lambda row, n: rest_ref.at[pl.ds(row - PIECE, n)], g_sem, 3)

    def local_copy(m):
        return pltpu.make_async_copy(w_refs[m], w_s.at[m, pl.ds(0, PIECE)], l_sem.at[m])

    XR = x_s.shape[1]
    steps = TOK // XR

    def x_in(n):
        return pltpu.make_async_copy(x_ref.at[pl.ds(n * XR, XR)], x_s.at[lax.rem(n, 2)], x_sem.at[lax.rem(n, 2)])

    x_in(0).start()
    for m in range(3):
        gathers[m].start_x()
    pl.when(first_chip)(wo.start_x)
    for m in range(3):
        gathers[m].own().start()
        local_copy(m).start()

    def norm(n, _):
        @pl.when(n + 1 < steps)
        def _():
            x_in(n + 1).start()

        x_in(n).wait()
        slot = lax.rem(n, 2)
        wide = x_s[slot].astype(F32)
        scale = lax.rsqrt(jnp.mean(wide * wide, -1, keepdims=True) + 1e-6)
        for j, p in enumerate((s, s1, s2, s3)):
            cols = pl.ds(pl.multiple_of(p * PIECE, PIECE), PIECE)
            a = x_s[slot, :, cols].astype(F32) * scale * gain_ref[:, cols].astype(F32)
            a_s[pl.ds(pl.multiple_of(n * XR, XR), XR), j * PIECE : (j + 1) * PIECE] = a.astype(BF16)

    lax.fori_loop(0, steps, norm, None)

    def head_cols(h):
        return pl.ds(pl.multiple_of(h * HEAD, HEAD), HEAD)

    gathers[0].own().wait_recv()
    local_copy(0).wait()

    def begin(n, _):
        gathers[0].pass_x(n)
        for h in range(HEADS // NCH):
            cols = head_cols(HEADS // NCH * n + h)

            for r in range(TOK // STRIP):
                rows = pl.ds(r * STRIP, STRIP)
                p_s[rows, cols] = _dot(a_s[rows, : 2 * PIECE], w_s[0, : 2 * PIECE, cols])

    lax.fori_loop(0, NCH, begin, None)

    def table(n, _):
        at = pl.ds(pl.multiple_of(n * FINE, FINE), FINE)
        fc, fs = far_ref[0, pl.ds(n, 1), :], far_ref[1, pl.ds(n, 1), :]
        cos_s[at, :] = fc * near_ref[0] - fs * near_ref[1]
        sin_s[at, :] = fs * near_ref[0] + fc * near_ref[1]

    lax.fori_loop(0, TOK // FINE, table, None)
    for n in range(NCH):
        gathers[0].pass_y(n)

    outs = (qt_ref, k_ref, vt_ref)
    here = pl.ds(pl.multiple_of(core * TOK, TOK), TOK)

    def stage(m):
        return k_s if m == 1 else t_s

    def out(m, n):
        return outs[m].at[n, here, :] if m == 1 else outs[m].at[n, :, here]

    def sent(m, n):
        slot = lax.rem(n, 2)
        return _remote(stage(m).at[slot], out(m, n), slot_sem.at[0, slot], to_sem.at[m, n], beside)

    def kept(m, n):
        slot = lax.rem(n, 2)
        return pltpu.make_async_copy(stage(m).at[2 + slot], out(m, n), slot_sem.at[1, slot])

    def ask(p):
        return _remote(qt_ref.at[:, :, _cols(_early(core, p))], ask_ref.at[p], as_sem.at[p], ar_sem.at[p], across)

    def make(m, h, slot):
        cols = head_cols(h)
        for r in range(TOK // STRIP):
            rows = pl.ds(r * STRIP, STRIP)
            if m == 0:
                t = p_s[rows, cols] + _dot(a_s[rows, 2 * PIECE :], w_s[m, 2 * PIECE :, cols])
            else:
                t = _dot(a_s[rows, :], w_s[m, :, cols])
            t = t.astype(BF16)
            if m < 2:
                t = t.astype(F32)
                lo, hi = t[:, : HEAD // 2], t[:, HEAD // 2 :]
                cos, sin = cos_s[rows, :], sin_s[rows, :]
                t = jnp.concatenate([lo * cos - hi * sin, hi * cos + lo * sin], axis=1).astype(BF16)
            if m == 1:
                k_s[slot, rows, :] = t
            else:
                t_s[slot, :, rows] = t.T

    for m in range(3):
        gathers[m].arrived()
        if m:
            gathers[m].own().wait_recv()
            local_copy(m).wait()

        def head(n, _):
            i = lax.rem(n, OWN)
            home = n >= OWN

            @pl.when((i >= 2) & jnp.logical_not(home))
            def _():
                sent(m, i - 2).wait_send()

            @pl.when((i >= 2) & home)
            def _():
                kept(m, i - 2).wait()

            if m < 2:

                @pl.when(home)
                def _():
                    for c in range(NCH // OWN):
                        gathers[m + 1].pass_y(i * (NCH // OWN) + c)

            make(m, lax.rem((1 - core) * OWN + n, HEADS), lax.rem(n, 2) + 2 * lax.div(n, OWN))

            @pl.when(home)
            def _():
                kept(m, i).start()

            @pl.when(jnp.logical_not(home))
            def _():
                sent(m, i).start()
                if m < 2:
                    for c in range(NCH // OWN):
                        gathers[m + 1].pass_x(i * (NCH // OWN) + c)

        lax.fori_loop(0, HEADS, head, None)
        for n in (OWN - 2, OWN - 1):
            sent(m, n).wait_send()
            kept(m, n).wait()
        if m == 0:

            @pl.when(jnp.logical_not(first_chip))
            def _():
                for p in range(EARLY):
                    ask(p).start()

    for g in gathers:
        g.left()
    for m in range(3):
        for n in range(OWN):
            sent(m, n).wait_recv()

    @pl.when(first_chip)
    def _():
        for n in range(NCH):
            wo.x(n).wait_send()
        for p in range(EARLY):
            ask(p).wait_recv()

    @pl.when(jnp.logical_not(first_chip))
    def _():
        for n in range(NCH):
            wo.x(n).wait_recv()
        for p in range(EARLY):
            ask(p).wait_send()


def project(x, gain, far, near, wq, wk, wv, wo):
    hbm, vmem = pl.BlockSpec(memory_space=pltpu.HBM), pl.BlockSpec(memory_space=pltpu.VMEM)
    dma = pltpu.SemaphoreType.DMA
    return pl.pallas_call(
        _project,
        in_specs=[hbm, vmem, vmem, vmem, hbm, hbm, hbm, hbm],
        out_specs=[hbm] * 5,
        out_shape=[
            jax.ShapeDtypeStruct((OWN, HEAD, CHIP), BF16),
            jax.ShapeDtypeStruct((OWN, CHIP, HEAD), BF16),
            jax.ShapeDtypeStruct((OWN, HEAD, CHIP), BF16),
            jax.ShapeDtypeStruct((EARLY, OWN, HEAD, STRIP), BF16),
            jax.ShapeDtypeStruct((3 * PIECE, D), BF16),
        ],
        scratch_shapes=[
            pltpu.VMEM((TOK, D), BF16),
            pltpu.VMEM((2, 256, D), BF16),
            pltpu.VMEM((3, D, D), BF16),
            pltpu.VMEM((TOK, D), F32),
            pltpu.VMEM((4, HEAD, TOK), BF16),
            pltpu.VMEM((4, TOK, HEAD), BF16),
            pltpu.VMEM((TOK, HEAD // 2), F32),
            pltpu.VMEM((TOK, HEAD // 2), F32),
            dma((2,)), dma((3,)), dma((2, 2)), dma((3, OWN)), dma((EARLY,)), dma((EARLY,)),
            *_gather_sems(4),
        ],
        compiler_params=pltpu.CompilerParams(collective_id=0, has_side_effects=True, vmem_limit_bytes=VMEM),
        cost_estimate=pl.CostEstimate(flops=6 * TOK * D * D, transcendentals=0, bytes_accessed=64 * 2**20),
        name="project",
    )(x, gain, far, near, wq, wk, wv, wo)


def _attend(qt_ref, k_ref, vt_ref, ask_ref, wo_ref, _, seen_ref, rest_ref,
            q_s, k_s, v_s, far_s, mix_s, top_s, part_s, lse_s, flse_s, seen_s, sa_s, sb_s,
            in_sem, q_sem, f_sem, qs_sem, qr_sem, ps_sem, pr_sem, ls_sem, lr_sem, slot_sem, to_sem, *g_sem):
    dp, s, core, s1, s2, _ = _places()
    beside, across, other = (dp, s1), (dp, s2), (1 - dp, s)
    first_chip = s < 2
    e = SCALE * LOG2E
    _greet((beside, across, other))
    wo = _Gather(wo_ref, lambda row, n: rest_ref.at[pl.ds(row - PIECE, n)], g_sem, 0)
    cols = _cols

    def early(p):
        return _early(core, p)

    def place(p):
        return jnp.where(p < NS // 2, (1 - core) * (NS // 2) + NS // 2 - 1 - p, core * (NS // 2) + NS - 1 - p)

    def ask(p):
        at = cols(early(p))
        return _remote(qt_ref.at[:, :, at], far_s.at[:, :, at], qs_sem.at[p], qr_sem.at[p], across)

    def asked(p):
        return pltpu.make_async_copy(ask_ref.at[p], far_s.at[:, :, cols(early(p))], f_sem.at[p])

    def answer(p):
        return [c for half in range(2) for c in answered(p, half)]

    def answered(p, half):
        slot, heads = lax.rem(p, 2), pl.ds(2 * half, 2)
        return (_remote(part_s.at[slot, heads], far_s.at[heads, :, cols(early(p))], ps_sem.at[slot, half], pr_sem.at[p, half], across),
                _remote(lse_s.at[slot, half], flse_s.at[p, half], ls_sem.at[slot, half], lr_sem.at[p, half], across))

    def q_in(p):
        slot = lax.rem(p, 2)
        return pltpu.make_async_copy(qt_ref.at[:, :, cols(place(p))], q_s.at[slot], q_sem.at[slot])

    def ours(t):
        return lax.div(t, NS // 2) == core

    def target(t):
        return seen_ref.at[pl.ds(core * OWN, OWN), cols(lax.rem(t, NS // 2))]

    def sent(t, slot):
        return _remote(seen_s.at[slot], target(t), slot_sem.at[slot], to_sem.at[lax.rem(t, NS // 2)], beside)

    def kept(t, slot):
        return pltpu.make_async_copy(seen_s.at[slot], target(t), slot_sem.at[slot])

    def hand(t, slot):
        @pl.when(ours(t))
        def _():
            kept(t, slot).start()

        @pl.when(jnp.logical_not(ours(t)))
        def _():
            sent(t, slot).start()

    def handed(t, slot):
        @pl.when(ours(t))
        def _():
            kept(t, slot).wait()

        @pl.when(jnp.logical_not(ours(t)))
        def _():
            sent(t, slot).wait_send()

    def pair_in(half):
        heads = pl.ds(2 * half, 2)
        return (pltpu.make_async_copy(k_ref.at[heads], k_s.at[heads], in_sem.at[half, 0]),
                pltpu.make_async_copy(vt_ref.at[heads], v_s.at[heads], in_sem.at[half, 1]))

    @pl.when(first_chip)
    def _():
        for p in range(EARLY):
            asked(p).start()

    for half in range(2):
        for c in pair_in(half):
            c.start()
    q_in(0).start()

    @pl.when(jnp.logical_not(first_chip))
    def _():
        for p in range(EARLY, NS):
            ask(p).start()
        wo.start_x()
        for n in range(NCH):
            wo.y(n).start()
            wo.d(n).start()

    wo.own().start()
    for c in pair_in(0):
        c.wait()

    @pl.when(jnp.logical_not(first_chip))
    def _():
        for c in pair_in(1):
            c.wait()

    ones = jnp.ones((8, STRIP), BF16)

    def clear(t, heads):
        for i in heads:
            top_s[i : i + 1, cols(t)] = jnp.full((1, STRIP), NEG, F32)
            mix_s[i, :, cols(t)] = jnp.zeros((HEAD + 8, STRIP), F32)

    def run(t, query, masked, count, heads=range(OWN)):
        def score(i, j, into):
            into[i] = _dot(k_s[i, cols(j), :], query(i))

        def fold(i, j, held, cut):
            sc = held[i]
            if cut:
                query_at, key_at = (lax.broadcasted_iota(jnp.int32, (STRIP, STRIP), n) for n in (1, 0))
                sc = jnp.where(query_at >= key_at, sc, HIDDEN)
            old = top_s[i : i + 1, cols(t)]
            top = jnp.maximum(old, sc.max(axis=0, keepdims=True))
            top_s[i : i + 1, cols(t)] = top
            weights = jnp.exp2((sc - top) * e).astype(BF16)
            keep = jnp.exp2((old - top) * e)
            val = jnp.concatenate([v_s[i, :, cols(j)], ones], axis=0)
            mix_s[i, :, cols(t)] = mix_s[i, :, cols(t)] * keep + _dot(val, weights)

        def step(j, held, after, into, cut=False):
            for i in heads:
                if after is not None:
                    score(i, after, into)
                fold(i, j, held, cut)

        def pair(n, _):
            step(2 * n, sa_s, 2 * n + 1, sb_s)
            step(2 * n + 1, sb_s, 2 * n + 2, sa_s)

        def single():
            step(count - 1, sa_s, None, None)

        def double():
            step(count - 2, sa_s, count - 1, sb_s)
            step(count - 1, sb_s, None, None)

        clear(t, heads)
        if masked:
            for i in heads:
                score(i, t, sb_s)
            step(t, sb_s, 0, sa_s, True)
            lax.fori_loop(0, lax.div(jnp.maximum(count - 1, 0), 2), pair, None)
            pl.when(lax.rem(count, 2) == 1)(single)
            pl.when((lax.rem(count, 2) == 0) & (count > 0))(double)
        else:
            for i in heads:
                score(i, 0, sa_s)
            lax.fori_loop(0, (count - 1) // 2, pair, None)
            double()

    def own(p):
        t, slot = place(p), lax.rem(p, 2)

        @pl.when(p + 1 < NS)
        def _():
            q_in(p + 1).start()

        q_in(p).wait()
        run(t, lambda i: q_s[slot, i], True, t)

    def cross(p):
        t = early(p)

        @pl.when(p < EARLY)
        def _():
            asked(p).wait()

        @pl.when(p >= EARLY)
        def _():
            ask(p).wait_recv()

        slot = lax.rem(p, 2)
        for half in range(2):
            heads = (2 * half, 2 * half + 1)
            if half:

                @pl.when(p == 0)
                def _():
                    for c in pair_in(1):
                        c.wait()

            run(t, lambda i: far_s[i, :, cols(t)], False, NS, heads)

            @pl.when(p >= 2)
            def _():
                for c in answered(p - 2, half):
                    c.wait_send()

            for i in heads:
                total = mix_s[i, HEAD : HEAD + 1, cols(t)]
                part_s[slot, i] = (mix_s[i, :HEAD, cols(t)] * (1 / total)).astype(BF16)
                lse_s[slot, half, i % 2 : i % 2 + 1, :] = top_s[i : i + 1, cols(t)] * SCALE + jnp.log(total)
            for c in answered(p, half):
                c.start()

    def finish(p):
        t, slot = place(p), lax.rem(p, 2)

        @pl.when(p >= 2)
        def _():
            handed(place(p - 2), slot)

        for i in range(OWN):
            total = mix_s[i, HEAD : HEAD + 1, cols(t)]
            seen_s[slot, i] = (mix_s[i, :HEAD, cols(t)] * (1 / total)).T.astype(BF16)
        hand(t, slot)

    def join(p):
        t, slot = early(p), lax.rem(p, 2)

        @pl.when(p >= 2)
        def _():
            handed(early(p - 2), slot)

        for i in range(OWN):
            total = mix_s[i, HEAD : HEAD + 1, cols(t)]
            mine = top_s[i : i + 1, cols(t)] * SCALE + jnp.log(total)
            theirs = flse_s[p, i // 2, i % 2 : i % 2 + 1, :]
            top = jnp.maximum(mine, theirs)
            wm, wt = jnp.exp(mine - top), jnp.exp(theirs - top)
            both = 1 / (wm + wt)
            mixed = mix_s[i, :HEAD, cols(t)] * (wm * both / total) + far_s[i, :, cols(t)].astype(F32) * (wt * both)
            seen_s[slot, i] = mixed.T.astype(BF16)
        hand(t, slot)

    def step(p, _):
        @pl.when(first_chip)
        def _():
            cross(p)

        own(p)

        @pl.when(first_chip)
        def _():
            finish(p)

    lax.fori_loop(0, NS, step, None)

    @pl.when(first_chip)
    def _():
        for n in range(NCH):
            wo.pass_x(n)

    for n in range(NCH):
        wo.pass_y(n)

    @pl.when(first_chip)
    def _():
        for p in (NS - 2, NS - 1):
            for c in answer(p):
                c.wait_send()
            handed(place(p), p % 2)

    @pl.when(jnp.logical_not(first_chip))
    def _():
        for p in range(EARLY, NS):
            ask(p).wait_send()
        for n in range(NCH):
            wo.x(n).wait_send()

        def merge(p, _):
            for c in answer(p):
                c.wait_recv()
            join(p)

        lax.fori_loop(0, NS, merge, None)
        for p in (NS - 2, NS - 1):
            handed(early(p), p % 2)

    for n in range(NS // 2):
        sent(n, 0).wait_recv()
    wo.own().wait_recv()
    wo.own().wait_send()
    wo.arrived()
    wo.passed()


def attend(qt, k, vt, asked, wo, rest):
    hbm = pl.BlockSpec(memory_space=pltpu.HBM)
    dma = pltpu.SemaphoreType.DMA
    return pl.pallas_call(
        _attend,
        in_specs=[hbm] * 6,
        out_specs=[hbm] * 2,
        input_output_aliases={5: 1},
        out_shape=[jax.ShapeDtypeStruct((HEADS, TOK, HEAD), BF16), jax.ShapeDtypeStruct((3 * PIECE, D), BF16)],
        scratch_shapes=[
            pltpu.VMEM((2, OWN, HEAD, STRIP), BF16),
            pltpu.VMEM((OWN, CHIP, HEAD), BF16),
            pltpu.VMEM((OWN, HEAD, CHIP), BF16),
            pltpu.VMEM((OWN, HEAD, CHIP), BF16),
            pltpu.VMEM((OWN, HEAD + 8, CHIP), F32),
            pltpu.VMEM((OWN, CHIP), F32),
            pltpu.VMEM((2, OWN, HEAD, STRIP), BF16),
            pltpu.VMEM((2, 2, OWN // 2, STRIP), F32),
            pltpu.VMEM((NS, 2, OWN // 2, STRIP), F32),
            pltpu.VMEM((2, OWN, STRIP, HEAD), BF16),
            pltpu.VMEM((OWN, STRIP, STRIP), F32),
            pltpu.VMEM((OWN, STRIP, STRIP), F32),
            dma((2, 2)), dma((2,)), dma((EARLY,)), dma((NS,)), dma((NS,)), dma((2, 2)), dma((NS, 2)), dma((2, 2)), dma((NS, 2)), dma((2,)),
            dma((NS // 2,)),
            *_gather_sems(1),
        ],
        compiler_params=pltpu.CompilerParams(collective_id=1, has_side_effects=True, vmem_limit_bytes=VMEM),
        cost_estimate=pl.CostEstimate(flops=6 * OWN * CHIP * CHIP * HEAD, transcendentals=OWN * CHIP * CHIP, bytes_accessed=64 * 2**20),
        name="attend",
    )(qt, k, vt, asked, wo, rest)


def _output(seen_ref, x_ref, wo_ref, rest_ref, y_ref, w_s, w_sem):
    _, s, _, s1, s2, s3 = _places()
    chunks = D // 512

    def w_in(n):
        at = pl.ds(n * 512, 512)
        return (pltpu.make_async_copy(wo_ref.at[:, at], w_s.at[pl.ds(0, PIECE), at], w_sem.at[n, 0]),
                pltpu.make_async_copy(rest_ref.at[:, at], w_s.at[pl.ds(PIECE, 3 * PIECE), at], w_sem.at[n, 1]))

    def rows(fetch):
        if fetch:
            for n in range(chunks):
                for c in w_in(n):
                    c.start()
        lhs = jnp.concatenate([seen_ref[p * 2 + i] for p in (s, s1, s2, s3) for i in range(2)], axis=1)
        for n in range(chunks):
            if fetch:
                for c in w_in(n):
                    c.wait()
            at = slice(n * 512, (n + 1) * 512)
            y_ref[:, at] = (x_ref[:, at].astype(F32) + _dot(lhs, w_s[:, at])).astype(BF16)

    pl.when(pl.program_id(0) == 0)(lambda: rows(True))
    pl.when(pl.program_id(0) > 0)(lambda: rows(False))


def output(seen, x, wo, rest):
    rows = 512
    hbm = pl.BlockSpec(memory_space=pltpu.HBM)
    return pl.pallas_call(
        _output,
        grid=(TOK // rows,),
        in_specs=[pl.BlockSpec((HEADS, rows, HEAD), lambda i: (0, i, 0)), pl.BlockSpec((rows, D), lambda i: (i, 0)), hbm, hbm],
        out_specs=pl.BlockSpec((rows, D), lambda i: (i, 0)),
        out_shape=jax.ShapeDtypeStruct((TOK, D), BF16),
        scratch_shapes=[pltpu.VMEM((D, D), BF16), pltpu.SemaphoreType.DMA((D // 512, 2))],
        compiler_params=pltpu.CompilerParams(dimension_semantics=("arbitrary",), vmem_limit_bytes=56 * 2**20),
        cost_estimate=pl.CostEstimate(flops=2 * TOK * D * D, transcendentals=0, bytes_accessed=32 * 2**20),
        name="output",
    )(seen, x, wo, rest)


def solution(mesh):
    def step(x, gain, wq, wk, wv, wo):
        s = lax.axis_index("sp")
        rate = THETA ** (-jnp.arange(HEAD // 2, dtype=F32) / (HEAD // 2))

        def table(place):
            angle = place.astype(F32)[:, None] * rate
            return jnp.stack([jnp.cos(angle), jnp.sin(angle)])

        far, near = table(s * TOK + FINE * jnp.arange(TOK // FINE)), table(jnp.arange(FINE))
        qt, k, vt, asked, rest = project(x, gain[None], far, near, wq, wk, wv, wo)
        seen, rest = attend(qt, k, vt, asked, wo, rest)
        return output(seen, x, wo, rest)

    tokens, whole = P(("dp", "sp"), None), P("sp", None)
    return jax.shard_map(
        step,
        mesh=mesh,
        in_specs=(tokens, P(None), whole, whole, whole, whole),
        out_specs=tokens,
        check_vma=False,
    )
```
